256 devices in a mesh: row: 32 (over x, z_lo, y), col: 8 (over z_hi, core).
Axes of the slice: x: 4, y: 4, z: 8 (z_hi: 4, z_lo: 2; z = z_hi * 2 + z_lo), core: 2. Of those that a mesh axis runs over, the one named last changes fastest.
Arguments:
- adj_tiles: bfloat16 [32, 8, 128, 128, 128], P('row', 'col'), may hold values from 0 to 1, as said below
- tile_rows: int32 [32, 8, 128], P('row', 'col'), may hold values from 0 to 7, as said below
- tile_cols: int32 [32, 8, 128], P('row', 'col'), may hold values from 0 to 31, as said below
- tile_count: int32 [32, 8], P('row', 'col'), may hold values from 1 to 128, as said below
- tile_depth: int32 [256, 128], P(('row', 'col')), may hold values from 1 to 7, as said below
- source_ids: int32 [128], replicated, may hold values from 0 to 32767
Outputs:
- path_sums: float32 [32768, 128], P(('row', 'col'))
- log_scales: float32 [6, 128], replicated
The draws below stay inside these ranges and needn't reach their ends.
Inputs may be any that keep to these rules, and one draw needn't show every extreme that they name: `adj_tiles`: every entry is 0 or 1. The live slots of a device are its first tile_count slots; at least one device holds 128 live slots. `tile_rows`: slots past a device's live count carry 0. `tile_cols`: slots past a device's live count carry 0. `tile_depth`: the value 6 + 1 marks a tile that takes path counts at every level.
All inputs are finite; a program needn't handle non-finite values.
Results may differ from the reference program's by a relative error of at most 0.0003.
Values may be sent and summed in bfloat16 or wider, within the bound.
A program may use at most 64 MiB of HBM per device.

```python
import jax
import jax.numpy as jnp
from jax import lax

TILE = 128
PANEL = 128
PIECE = 128
KMAX = 128
LEVELS = 6
VERTICES = 32768
VTILES = 256
DEST_TILES = 8
SRC_TILES = 32
N_ROW = 32
N_COL = 8


def tile_lists(key):
    grid_shape = (N_ROW, N_COL)
    light = jax.random.randint(jax.random.fold_in(key, 11), grid_shape, KMAX // 4, KMAX // 2 + 1)
    heavy = jax.random.randint(jax.random.fold_in(key, 12), grid_shape, 0, 4) == 0
    loaded = jax.random.randint(jax.random.fold_in(key, 13), grid_shape, 3 * KMAX // 4, KMAX + 1)
    counts = jnp.where(heavy, loaded, light)
    chosen = jax.random.randint(jax.random.fold_in(key, 14), (), 0, N_ROW * N_COL)
    device_ids = jnp.arange(N_ROW * N_COL, dtype=jnp.int32).reshape(grid_shape)
    counts = jnp.where(device_ids == chosen, KMAX, counts).astype(jnp.int32)
    slot_ids = jnp.arange(KMAX, dtype=jnp.int32)[None, None, :]
    live_slots = slot_ids < counts[:, :, None]
    dest_ids = jax.random.randint(jax.random.fold_in(key, 15), grid_shape + (KMAX,), 0, DEST_TILES)
    src_ids = jax.random.randint(jax.random.fold_in(key, 16), grid_shape + (KMAX,), 0, SRC_TILES)
    dest_ids = jnp.where(live_slots, dest_ids, 0).astype(jnp.int32)
    src_ids = jnp.where(live_slots, src_ids, 0).astype(jnp.int32)
    return (counts, dest_ids, src_ids)


def draw_adj_tiles(key, part):
    counts, dest_ids, src_ids = tile_lists(key)
    piece_tiles = PIECE // TILE
    row_index = jnp.arange(N_ROW, dtype=jnp.int32)[:, None, None]
    col_index = jnp.arange(N_COL, dtype=jnp.int32)[None, :, None]
    dest_global = (row_index * (N_COL * piece_tiles) + dest_ids).astype(jnp.int32)
    src_global = ((src_ids // piece_tiles * N_COL + col_index) * piece_tiles + src_ids % piece_tiles).astype(jnp.int32)
    log_weight = jax.random.uniform(jax.random.fold_in(key, 33), (VTILES, TILE), jnp.float32, jnp.log(0.3), jnp.log(1.0))
    vertex_weight = jnp.exp(log_weight)
    dest_weight = jnp.take(vertex_weight, dest_global, axis=0)
    src_weight = jnp.take(vertex_weight, src_global, axis=0)
    pair_weight = dest_weight[:, :, :, :, None] * src_weight[:, :, :, None, :]
    slot_shape = (N_ROW, N_COL, KMAX, 1, 1)
    log_density = jax.random.uniform(jax.random.fold_in(key, 31), slot_shape, jnp.float32, jnp.log(0.15), jnp.log(0.6))
    density = jnp.exp(log_density)
    offset = jax.random.randint(jax.random.fold_in(key, 34), slot_shape, 0, TILE)
    positions = jnp.arange(TILE, dtype=jnp.int32)
    spread = positions[None, :] - positions[:, None]
    inside = (spread[None, None, None, :, :] - offset) % TILE < TILE // 4
    rate = jnp.where(inside, jnp.minimum(1.0, 4.0 * density * pair_weight), 0.15 * pair_weight)
    coins = jax.random.uniform(jax.random.fold_in(key, 32), (N_ROW, N_COL, KMAX, TILE, TILE), jnp.float32)
    return (coins < rate).astype(jnp.float32).astype(jnp.bfloat16)


def draw_tile_count(key, part):
    return tile_lists(key)[0]


def draw_tile_rows(key, part):
    return tile_lists(key)[1]


def draw_tile_cols(key, part):
    return tile_lists(key)[2]


def draw_tile_depth(key, part):
    base_level = jax.random.randint(jax.random.fold_in(key, 21), (VTILES, 1), 0, LEVELS + 1)
    offset = jax.random.randint(jax.random.fold_in(key, 22), (VTILES, PANEL), 0, LEVELS + 1)
    return (1 + jnp.maximum(base_level, offset)).astype(jnp.int32)


def place_ends(values, own_key, low, largest):
    longest = values.shape.index(max(values.shape))
    spots = []
    for shift in (0, 1):
        where = [jax.random.randint(jax.random.fold_in(own_key, axis), (), 0, length) for axis, length in enumerate(values.shape)]
        where[longest] = (where[longest] + shift) % values.shape[longest]
        spots.append(tuple(where))
    return values.at[spots[0]].set(low).at[spots[1]].set(largest)


def setup_inputs(seed: int = 0) -> dict:
    keys = jax.random.split(jax.random.key(seed), 7)
    adj_tiles = draw_adj_tiles(jax.random.fold_in(keys[6], 71), 0)
    tile_rows = draw_tile_rows(jax.random.fold_in(keys[6], 71), 0)
    tile_cols = draw_tile_cols(jax.random.fold_in(keys[6], 71), 0)
    tile_count = draw_tile_count(jax.random.fold_in(keys[6], 71), 0)
    tile_depth = draw_tile_depth(jax.random.fold_in(keys[6], 71), 0)
    source_ids = place_ends(jax.random.randint(keys[5], (PANEL,), 0, VERTICES), jax.random.fold_in(keys[5], 1), 0, VERTICES - 1).astype(jnp.int32)
    return dict(adj_tiles=adj_tiles, tile_rows=tile_rows, tile_cols=tile_cols, tile_count=tile_count, tile_depth=tile_depth, source_ids=source_ids)


EPSILON = 1e-06

def reference(adj_tiles, tile_rows, tile_cols, tile_count, tile_depth, source_ids):
    piece_tiles = PIECE // TILE
    tile_total = VERTICES // TILE
    row_slots = N_COL * KMAX
    slot_ids = jnp.arange(KMAX, dtype=jnp.int32)[None, None, :]
    row_index = jnp.arange(N_ROW, dtype=jnp.int32)[:, None, None]
    col_index = jnp.arange(N_COL, dtype=jnp.int32)[None, :, None]
    dest_tile = (row_index * (N_COL * piece_tiles) + tile_rows).reshape(-1).astype(jnp.int32)
    src_tile = ((tile_cols // piece_tiles * N_COL + col_index) * piece_tiles + tile_cols % piece_tiles).reshape(-1).astype(jnp.int32)
    live_slots = (slot_ids < tile_count[:, :, None]).astype(jnp.float32).reshape(-1)
    flat_tiles = adj_tiles.reshape(N_ROW * row_slots, TILE, TILE)

    def product(frontier):

        def one_row(summed, row_number):
            first_slot = (row_number * row_slots).astype(jnp.int32)
            block_part = lax.dynamic_slice_in_dim(flat_tiles, first_slot, row_slots, 0).astype(jnp.float32)
            dest_part = lax.dynamic_slice_in_dim(dest_tile, first_slot, row_slots, 0)
            src_part = lax.dynamic_slice_in_dim(src_tile, first_slot, row_slots, 0)
            weights = lax.dynamic_slice_in_dim(live_slots, first_slot, row_slots, 0)
            picked = jnp.take(frontier, src_part, axis=0).astype(jnp.float32)
            slot_terms = jnp.einsum('kij,kjs->kis', block_part, picked, precision=lax.Precision.HIGHEST)
            slot_terms = slot_terms * weights[:, None, None]
            return (summed.at[dest_part].add(slot_terms), None)
        zero_sums = jnp.zeros((tile_total, TILE, PANEL), jnp.float32)
        summed, unused = lax.scan(one_row, zero_sums, jnp.arange(N_ROW, dtype=jnp.int32))
        return summed
    vertex_ids = jnp.arange(VERTICES, dtype=jnp.int32)
    start_panel = (vertex_ids[:, None] == source_ids[None, :]).astype(jnp.float32)
    path_sums = start_panel
    frontier = start_panel.astype(jnp.bfloat16)
    log_scales = []
    for level_index in range(1, LEVELS + 1):
        summed = product(frontier.reshape(tile_total, TILE, PANEL))
        reached = (tile_depth >= level_index).astype(jnp.float32)
        raw_paths = (summed * reached[:, None, :]).reshape(VERTICES, PANEL)
        mean_square = lax.optimization_barrier(jnp.sum(raw_paths * raw_paths, axis=0)) / VERTICES + EPSILON
        scaled = raw_paths * lax.rsqrt(mean_square)
        path_sums = path_sums + scaled
        log_scales.append(0.5 * jnp.log(mean_square))
        frontier = scaled.astype(jnp.bfloat16)
    return (path_sums, jnp.stack(log_scales))
```

```python
import jax
import jax.numpy as jnp
from jax import lax
from jax.experimental import pallas as pl
from jax.experimental.pallas import tpu as pltpu
from jax.sharding import PartitionSpec as P

MESH = pl.DeviceIdType.MESH
TILE = 128
PANEL = 128
LEVELS = 6
KMAX = 128
DESTS = 8
SRCS = 32
N_ROW = 32
N_COL = 8
VERTICES = 32768
EPSILON = 1e-06
SHRINK = 2.0**-10
CHUNK = 4
CHUNK_K = CHUNK * TILE
LOADS = 8
LOAD_SLOTS = KMAX // LOADS


def place_of(x, z_lo, y):
    return z_lo * 16 + (1 - z_lo) * (x * 4 + y) + z_lo * (y * 4 + x)


def row_of(x, z_lo, y):
    return x * 8 + z_lo * 4 + y


def densify(count_ref, rows_ref, cols_ref, tiles_hbm, dense_ref, tiles, load_sem):
    count = count_ref[0]

    def load(part):
        slots = pl.ds(part * LOAD_SLOTS, LOAD_SLOTS)
        return pltpu.make_async_copy(tiles_hbm.at[slots], tiles.at[slots], load_sem.at[part])

    for part in range(LOADS):
        load(part).start()

    @pl.loop(0, DESTS * TILE // 16)
    def _(block):
        rows = pl.ds(pl.multiple_of(block * 16, 16), 16)
        dense_ref[rows, :] = jnp.zeros((16, SRCS * TILE), jnp.bfloat16)

    for part in range(LOADS):
        load(part).wait()

        @pl.loop(part * LOAD_SLOTS, jnp.minimum(count, (part + 1) * LOAD_SLOTS))
        def _(slot):
            dest = rows_ref[slot]
            row = cols_ref[slot]
            place = place_of(row // 8, (row // 4) % 2, row % 4)
            rows = pl.ds(pl.multiple_of(dest * TILE, TILE), TILE)
            columns = pl.ds(pl.multiple_of(place * TILE, TILE), TILE)
            dense_ref[rows, columns] = dense_ref[rows, columns] + tiles[slot]


def levels_kernel(
    dense,
    depth_ref,
    ids_ref,
    sums_ref,
    logs_ref,
    panel,
    partial,
    from_core,
    combined,
    from_z,
    paths,
    squares,
    squares_col,
    squares_row,
    tile_send,
    tile_recv,
    core_send,
    core_recv,
    z_send,
    z_recv,
    col_send,
    col_recv,
    row_send,
    row_recv,
):
    r = lax.axis_index("row")
    c = lax.axis_index("col")
    x, z_lo, y = r // 8, (r // 4) % 2, r % 4
    z_hi, core = c // 2, c % 2
    my_place = place_of(x, z_lo, y)

    barrier = pltpu.get_barrier_semaphore()

    @pl.loop(1, N_ROW)
    def _(step):
        pl.semaphore_signal(
            barrier, inc=1, device_id={"row": (r + step) % N_ROW, "col": c}, device_id_type=MESH
        )

    @pl.loop(1, N_COL)
    def _(step):
        pl.semaphore_signal(
            barrier, inc=1, device_id={"row": r, "col": (c + step) % N_COL}, device_id_type=MESH
        )

    def multiply(chunk, first):
        columns = pl.ds(pl.multiple_of(chunk * CHUNK_K, CHUNK_K), CHUNK_K)

        def run(buffer):
            source = panel[buffer, pl.ds(pl.multiple_of(chunk * CHUNK, CHUNK), CHUNK)].reshape(CHUNK_K, PANEL)
            for part in range(4):
                product = jnp.dot(
                    dense[part * 256 : (part + 1) * 256, columns], source, preferred_element_type=jnp.float32
                ).reshape(2, TILE, PANEL)
                if first:
                    partial[part * 2 : part * 2 + 2] = product
                else:
                    partial[part * 2 : part * 2 + 2] += product

        return run

    def tile_copy(buffer, place, to_x, to_z, to_y):
        return pltpu.make_async_remote_copy(
            src_ref=panel.at[buffer, place],
            dst_ref=panel.at[buffer, place],
            send_sem=tile_send,
            recv_sem=tile_recv.at[buffer, place],
            device_id={"row": row_of(to_x, to_z, to_y), "col": c},
            device_id_type=MESH,
        )

    def wait_tile(buffer, place):
        pltpu.make_async_copy(
            panel.at[buffer, place], panel.at[buffer, place], tile_recv.at[buffer, place]
        ).wait()

    x_up, x_down, x_far = (x + 1) % 4, (x + 3) % 4, (x + 2) % 4
    y_up, y_down, y_far = (y + 1) % 4, (y + 3) % 4, (y + 2) % 4

    def gather_start(buffer):
        for step in range(1, 8):
            z_step, step_4 = step // 4, step % 4
            tile_copy(
                buffer,
                my_place,
                (x + step_4 * z_lo) % 4,
                (z_lo + z_step) % 2,
                (y + step_4 * (1 - z_lo)) % 4,
            ).start()

    def gather_forward(buffer):
        for step in range(4):
            place_a = place_of(x, 0, (y + step) % 4)
            place_b = place_of((x + step) % 4, 1, y)
            if step == 0:
                pl.when(z_lo == 1)(lambda: wait_tile(buffer, place_a))
            else:
                wait_tile(buffer, place_a)
            tile_copy(buffer, place_a, x_up, z_lo, y).start()
            tile_copy(buffer, place_a, x_down, z_lo, y).start()
            if step == 0:
                pl.when(z_lo == 0)(lambda: wait_tile(buffer, place_b))
            else:
                wait_tile(buffer, place_b)
            tile_copy(buffer, place_b, x, z_lo, y_up).start()
            tile_copy(buffer, place_b, x, z_lo, y_down).start()
        multiply(x, True)(buffer)
        multiply(4 + y, False)(buffer)
        for step in range(4):
            row_a = (y + step) % 4
            row_b = (x + step) % 4
            up_a, down_a = place_of(x_down, 0, row_a), place_of(x_up, 0, row_a)
            up_b, down_b = place_of(row_b, 1, y_down), place_of(row_b, 1, y_up)
            for place in (up_a, down_a, up_b, down_b):
                wait_tile(buffer, place)
            even_a = row_a % 2 == 0
            tile_copy(
                buffer, jnp.where(even_a, up_a, down_a), jnp.where(even_a, x_up, x_down), z_lo, y
            ).start()
            even_b = row_b % 2 == 0
            tile_copy(
                buffer, jnp.where(even_b, up_b, down_b), x, z_lo, jnp.where(even_b, y_up, y_down)
            ).start()
        multiply(x_down, False)(buffer)
        multiply(x_up, False)(buffer)
        multiply(4 + y_down, False)(buffer)
        multiply(4 + y_up, False)(buffer)
        for step in range(4):
            wait_tile(buffer, place_of(x_far, 0, (y + step) % 4))
            wait_tile(buffer, place_of((x + step) % 4, 1, y_far))

    def core_copy(buffer, part):
        return pltpu.make_async_remote_copy(
            src_ref=partial.at[part * 2 + 1 - core],
            dst_ref=from_core.at[buffer, part],
            send_sem=core_send.at[part],
            recv_sem=core_recv.at[buffer, part],
            device_id={"row": r, "col": z_hi * 2 + 1 - core},
            device_id_type=MESH,
        )

    def z_copy(buffer, step):
        to = (z_hi + step) % 4
        return pltpu.make_async_remote_copy(
            src_ref=combined.at[step - 1],
            dst_ref=from_z.at[buffer, step - 1],
            send_sem=z_send.at[step - 1],
            recv_sem=z_recv.at[buffer, step - 1],
            device_id={"row": r, "col": to * 2 + core},
            device_id_type=MESH,
        )

    def reduce_level(level, buffer, out):
        for part in range(4):
            core_copy(buffer, part).start()
        for step in (2, 1, 3):
            to = (z_hi + step) % 4
            core_copy(buffer, to).wait_recv()
            combined[step - 1] = partial[to * 2 + core] + from_core[buffer, to]
            z_copy(buffer, step).start()
        core_copy(buffer, z_hi).wait_recv()
        mine = partial[z_hi * 2 + core] + from_core[buffer, z_hi]
        for step in (1, 3, 2):
            z_copy(buffer, step).wait_recv()
            mine = mine + from_z[buffer, step - 1]
        raw = jnp.where(depth_ref[...] >= level, mine, 0.0)
        paths[level - 1] = raw
        squares[pl.ds(level - 1, 1), :] = jnp.sum(raw * raw, axis=0, keepdims=True)
        if out is not None:
            panel[out, my_place] = (raw * SHRINK).astype(jnp.bfloat16)

    def drain(buffer):
        for part in range(4):
            core_copy(buffer, part).wait_send()
        for step in (1, 2, 3):
            z_copy(buffer, step).wait_send()

    squares[...] = jnp.zeros_like(squares)

    @pl.loop(0, SRCS)
    def _(row):
        place = place_of(row // 8, (row // 4) % 2, row % 4)
        vertex = (row * N_COL + c) * TILE + lax.broadcasted_iota(jnp.int32, (TILE, PANEL), 0)
        panel[0, place] = (vertex == ids_ref[...]).astype(jnp.float32).astype(jnp.bfloat16)

    multiply(0, True)(0)

    @pl.loop(1, 8)
    def _(chunk):
        multiply(chunk, False)(0)

    pl.semaphore_wait(barrier, N_ROW + N_COL - 2)
    reduce_level(1, 1, 1)

    @pl.loop(2, LEVELS + 1)
    def _(level):
        buffer = (level + 1) % 2
        gather_start(buffer)
        drain(0)
        gather_forward(buffer)
        multiply(x_far, False)(buffer)
        multiply(4 + y_far, False)(buffer)
        sent = panel.at[buffer, pl.ds(0, SRCS - 1)]
        pltpu.make_async_copy(sent, sent, tile_send).wait()
        reduce_level(level, 1 - buffer, 1 - buffer)

    drain(0)

    def col_copy(to):
        return pltpu.make_async_remote_copy(
            src_ref=squares,
            dst_ref=squares_col.at[c],
            send_sem=col_send,
            recv_sem=col_recv.at[c],
            device_id={"row": r, "col": to},
            device_id_type=MESH,
        )

    def row_copy(to):
        return pltpu.make_async_remote_copy(
            src_ref=squares,
            dst_ref=squares_row.at[r],
            send_sem=row_send,
            recv_sem=row_recv.at[r],
            device_id={"row": to, "col": c},
            device_id_type=MESH,
        )

    @pl.loop(1, N_COL)
    def _(step):
        col_copy((c + step) % N_COL).start()

    squares_col[c] = squares[...]

    @pl.loop(1, N_COL)
    def _(step):
        source = (c + step) % N_COL
        pltpu.make_async_copy(squares_col.at[source], squares_col.at[source], col_recv.at[source]).wait()

    sent_col = squares_col.at[pl.ds(0, N_COL - 1)]
    pltpu.make_async_copy(sent_col, sent_col, col_send).wait()
    squares[...] = jnp.sum(squares_col[...], axis=0)

    @pl.loop(1, N_ROW)
    def _(step):
        row_copy((r + step) % N_ROW).start()

    squares_row[r] = squares[...]

    @pl.loop(1, N_ROW)
    def _(step):
        source = (r + step) % N_ROW
        pltpu.make_async_copy(squares_row.at[source], squares_row.at[source], row_recv.at[source]).wait()

    sent_row = squares_row.at[pl.ds(0, N_ROW - 1)]
    pltpu.make_async_copy(sent_row, sent_row, row_send).wait()
    totals = jnp.sum(squares_row[...], axis=0)

    position = r * N_COL + c
    vertex = position * TILE + lax.broadcasted_iota(jnp.int32, (TILE, PANEL), 0)
    sums = (vertex == ids_ref[...]).astype(jnp.float32)
    kappa = jnp.ones((1, PANEL), jnp.float32)
    for level in range(LEVELS):
        mean_square = totals[level : level + 1] / VERTICES / kappa / kappa + EPSILON
        scale = kappa * jnp.sqrt(mean_square)
        sums = sums + paths[level] * (1.0 / scale)
        logs_ref[level : level + 1, :] = 0.5 * jnp.log(mean_square)
        kappa = scale * SHRINK
    sums_ref[...] = sums


def local(adj_tiles, tile_rows, tile_cols, tile_count, tile_depth, source_ids):
    smem = pl.BlockSpec(memory_space=pltpu.SMEM)
    vmem = pl.BlockSpec(memory_space=pltpu.VMEM)
    dense = pl.pallas_call(
        densify,
        out_shape=jax.ShapeDtypeStruct((DESTS * TILE, SRCS * TILE), jnp.bfloat16),
        in_specs=[smem, smem, smem, pl.BlockSpec(memory_space=pl.ANY)],
        out_specs=vmem,
        scratch_shapes=[
            pltpu.VMEM((KMAX, TILE, TILE), jnp.bfloat16),
            pltpu.SemaphoreType.DMA((LOADS,)),
        ],
        compiler_params=pltpu.CompilerParams(vmem_limit_bytes=24 * 2**20),
        name="densify",
    )(tile_count[0], tile_rows[0, 0], tile_cols[0, 0], adj_tiles[0, 0])
    return pl.pallas_call(
        levels_kernel,
        out_shape=(
            jax.ShapeDtypeStruct((TILE, PANEL), jnp.float32),
            jax.ShapeDtypeStruct((LEVELS, PANEL), jnp.float32),
        ),
        in_specs=[vmem, vmem, vmem],
        out_specs=(vmem, vmem),
        scratch_shapes=[
            pltpu.VMEM((2, SRCS, TILE, PANEL), jnp.bfloat16),
            pltpu.VMEM((DESTS, TILE, PANEL), jnp.float32),
            pltpu.VMEM((2, 4, TILE, PANEL), jnp.float32),
            pltpu.VMEM((3, TILE, PANEL), jnp.float32),
            pltpu.VMEM((2, 3, TILE, PANEL), jnp.float32),
            pltpu.VMEM((LEVELS, TILE, PANEL), jnp.float32),
            pltpu.VMEM((8, PANEL), jnp.float32),
            pltpu.VMEM((N_COL, 8, PANEL), jnp.float32),
            pltpu.VMEM((N_ROW, 8, PANEL), jnp.float32),
            pltpu.SemaphoreType.DMA,
            pltpu.SemaphoreType.DMA((2, SRCS)),
            pltpu.SemaphoreType.DMA((4,)),
            pltpu.SemaphoreType.DMA((2, 4)),
            pltpu.SemaphoreType.DMA((3,)),
            pltpu.SemaphoreType.DMA((2, 3)),
            pltpu.SemaphoreType.DMA,
            pltpu.SemaphoreType.DMA((N_COL,)),
            pltpu.SemaphoreType.DMA,
            pltpu.SemaphoreType.DMA((N_ROW,)),
        ],
        compiler_params=pltpu.CompilerParams(
            collective_id=0, has_side_effects=True, vmem_limit_bytes=32 * 2**20
        ),
        name="levels",
    )(dense, tile_depth, source_ids.reshape(1, PANEL))


def solution(mesh):
    in_specs = (
        P("row", "col", None, None, None),
        P("row", "col", None),
        P("row", "col", None),
        P("row", "col"),
        P(("row", "col"), None),
        P(),
    )
    out_specs = (P(("row", "col"), None), P())
    return jax.shard_map(local, mesh=mesh, in_specs=in_specs, out_specs=out_specs, check_vma=False)
```

```python
import jax
import jax.numpy as jnp
from jax import lax
from jax.experimental import pallas as pl
from jax.experimental.pallas import tpu as pltpu
from jax.sharding import PartitionSpec as P

MESH = pl.DeviceIdType.MESH
TILE = 128
HALF = 64
PANEL = 128
LEVELS = 6
KMAX = 128
DESTS = 8
SRCS = 32
N_ROW = 32
N_COL = 8
VERTICES = 32768
EPSILON = 1e-06
SHRINK_BITS = 10
SHRINK = 2.0**-SHRINK_BITS
GROWTH_BITS = 17
CODES = 65000.0
ZERO_CODE = -32768
LOADS = 8
LOAD_SLOTS = KMAX // LOADS
BLOCK = 256
OTHER, OWN = 0, 2


def place_of(x, z_lo, y):
    return (x * 4 + y) * 2 + z_lo


def row_of(x, z_lo, y):
    return x * 8 + z_lo * 4 + y


def densify(count_hbm, rows_hbm, cols_hbm, tiles_hbm, dense_ref, count_ref, rows_ref, cols_ref, tiles, small_sem, load_sem):
    core = lax.axis_index("col") % 2

    def load(part):
        slots = pl.ds(part * LOAD_SLOTS, LOAD_SLOTS)
        return pltpu.make_async_copy(tiles_hbm.at[0, 0, slots], tiles.at[slots], load_sem.at[part])

    small = (
        pltpu.make_async_copy(count_hbm, count_ref, small_sem.at[0]),
        pltpu.make_async_copy(rows_hbm, rows_ref, small_sem.at[1]),
        pltpu.make_async_copy(cols_hbm, cols_ref, small_sem.at[2]),
    )
    for copy in small:
        copy.start()
    for part in range(LOADS):
        load(part).start()

    @pl.loop(0, DESTS * TILE // 16)
    def _(block):
        rows = pl.ds(pl.multiple_of(block * 16, 16), 16)
        dense_ref[rows, :] = jnp.zeros((16, SRCS * TILE), jnp.bfloat16)

    for copy in small:
        copy.wait()
    count = count_ref[0, 0]
    for part in range(LOADS):
        load(part).wait()

        @pl.loop(part * LOAD_SLOTS, jnp.minimum(count, (part + 1) * LOAD_SLOTS))
        def _(slot):
            dest = rows_ref[0, 0, slot]
            row = cols_ref[0, 0, slot]
            place = place_of(row // 8, (row // 4) % 2, row % 4)
            block = jnp.where(dest % 2 == core, OWN, OTHER)
            columns = pl.ds(pl.multiple_of(place * TILE, TILE), TILE)
            for half in range(2):
                start = (block + half) * BLOCK + (dest // 2) * HALF
                rows = pl.ds(pl.multiple_of(start, HALF), HALF)
                dense_ref[rows, columns] = (
                    dense_ref[rows, columns] + tiles[slot, half * HALF : (half + 1) * HALF]
                )


def levels_kernel(
    dense,
    depth_ref,
    ids_ref,
    sums_ref,
    logs_ref,
    panel,
    partial,
    from_core,
    codes,
    from_z,
    paths,
    early,
    early_z,
    early_xy,
    last,
    last_z,
    last_xy,
    tile_send,
    tile_recv,
    core_send,
    core_recv,
    z_send,
    z_recv,
    norm_send,
    norm_recv,
):
    r = lax.axis_index("row")
    c = lax.axis_index("col")
    x, z_lo, y = r // 8, (r // 4) % 2, r % 4
    z_hi, core = c // 2, c % 2
    my_place = place_of(x, z_lo, y)

    barrier = pltpu.get_barrier_semaphore()

    @pl.loop(1, N_ROW)
    def _(step):
        pl.semaphore_signal(
            barrier, inc=1, device_id={"row": (r + step) % N_ROW, "col": c}, device_id_type=MESH
        )

    @pl.loop(1, N_COL)
    def _(step):
        to = (c + step) % N_COL
        pl.semaphore_signal(barrier, inc=1, device_id={"row": r, "col": to}, device_id_type=MESH)
        pl.semaphore_signal(
            barrier, inc=1, device_id={"row": row_of(x, 1 - z_lo, y), "col": to}, device_id_type=MESH
        )

    def product(buffer, chunks, block):
        rows = slice(block * BLOCK, (block + 1) * BLOCK)
        total = None
        for at_x, at_y in chunks:
            index = at_x * 4 + at_y
            columns = pl.ds(pl.multiple_of(index * 2 * TILE, 2 * TILE), 2 * TILE)
            source = panel[buffer, pl.ds(index * 2, 2)].reshape(2 * TILE, PANEL)
            term = jnp.dot(dense[rows, columns], source, preferred_element_type=jnp.float32)
            total = term if total is None else total + term
        return total

    def half_of(buffer, place, half):
        return panel.at[buffer, place, pl.ds(half * HALF, HALF)]

    def tile_copy(buffer, place, half, to_x, to_z, to_y):
        return pltpu.make_async_remote_copy(
            src_ref=half_of(buffer, place, half),
            dst_ref=half_of(buffer, place, half),
            send_sem=tile_send,
            recv_sem=tile_recv.at[buffer, half, place],
            device_id={"row": row_of(to_x, to_z, to_y), "col": c},
            device_id_type=MESH,
        )

    def wait_tile(buffer, place, half):
        ref = half_of(buffer, place, half)
        pltpu.make_async_copy(ref, ref, tile_recv.at[buffer, half, place]).wait()

    def at(half, along, across, z):
        ahead, side = ((x, y), (y, x))[half]
        ahead, side = (ahead + along) % 4, (side + across) % 4
        return (ahead, (z_lo + z) % 2, side) if half == 0 else (side, (z_lo + z) % 2, ahead)

    def plane_start(buffer, half):
        for along in (1, 3):
            tile_copy(buffer, my_place, half, *at(half, along, 0, 0)).start()
        for across, z in ((2, 1), (2, 0), (1, 1), (3, 1), (1, 0), (3, 0), (0, 1)):
            tile_copy(buffer, my_place, half, *at(half, 0, across, z)).start()

    def forward_plane(buffer, across, z):
        for half in range(2):
            place = place_of(*at(half, 0, across, z))
            wait_tile(buffer, place, half)
            for along in (1, 3):
                tile_copy(buffer, place, half, *at(half, along, 0, 0)).start()

    def forward_ring(buffer, across, z):
        for half in range(2):
            below = place_of(*at(half, 3, across, z))
            above = place_of(*at(half, 1, across, z))
            wait_tile(buffer, below, half)
            wait_tile(buffer, above, half)
            side = ((y, x)[half] + across) % 2
            x_up, _, y_up = at(half, 1, 0, 0)
            x_down, _, y_down = at(half, 3, 0, 0)
            even = side == 0
            tile_copy(
                buffer,
                jnp.where(even, below, above),
                half,
                jnp.where(even, x_up, x_down),
                z_lo,
                jnp.where(even, y_up, y_down),
            ).start()

    def wait_far(buffer, half, across):
        for z in range(2):
            wait_tile(buffer, place_of(*at(half, 2, across, z)), half)

    def spot(step_x, step_y):
        return (x + step_x) % 4, (y + step_y) % 4

    def gather(buffer, wait_sends):
        with jax.named_scope("fwd_plane"):
            forward_plane(buffer, 0, 1)
            forward_ring(buffer, 0, 0)
            for across, z in ((1, 0), (3, 0), (1, 1), (3, 1), (2, 0), (2, 1)):
                forward_plane(buffer, across, z)
        with jax.named_scope("fwd_ring"):
            for across, z in ((0, 1), (1, 0), (3, 0), (1, 1), (3, 1), (2, 0), (2, 1)):
                forward_ring(buffer, across, z)
        with jax.named_scope("mm_near"):
            wait_sends()
            near = [spot(i, j) for i in (0, 1, 3) for j in (0, 1, 3)]
            for block in range(4):
                partial[block] = product(buffer, near, block)
        with jax.named_scope("far_one"):
            for across in (0, 1):
                for half in range(2):
                    wait_far(buffer, half, across)
        with jax.named_scope("mm_one"):
            chunks = [spot(2, 0), spot(0, 2), spot(2, 1), spot(1, 2)]
            for block in range(4):
                partial[block] += product(buffer, chunks, block)
        with jax.named_scope("far_two"):
            for across in (3, 2):
                for half in range(2):
                    wait_far(buffer, half, across)
        return [spot(2, 3), spot(3, 2), spot(2, 2)]

    def core_copy(buffer, half):
        return pltpu.make_async_remote_copy(
            src_ref=partial.at[OTHER + half],
            dst_ref=from_core.at[buffer, half],
            send_sem=core_send.at[half],
            recv_sem=core_recv.at[buffer, half],
            device_id={"row": r, "col": z_hi * 2 + 1 - core},
            device_id_type=MESH,
        )

    def z_copy(buffer, half, step):
        return pltpu.make_async_remote_copy(
            src_ref=codes.at[half, step - 1],
            dst_ref=from_z.at[buffer, half, step - 1],
            send_sem=z_send.at[half, step - 1],
            recv_sem=z_recv.at[buffer, half, step - 1],
            device_id={"row": r, "col": ((z_hi + step) % 4) * 2 + core},
            device_id_type=MESH,
        )

    def code_scale(level):
        before = (jnp.zeros((1, PANEL), jnp.int32) + (level - 1)).astype(jnp.float32)
        steps = CODES / (GROWTH_BITS * (before + 1.0) + 0.5)
        middle = 0.5 * (GROWTH_BITS + (GROWTH_BITS - 2 * SHRINK_BITS) * before)
        return steps, middle

    def both_cores(buffer, half, part):
        rows = pl.ds(pl.multiple_of(part * HALF, HALF), HALF)
        return partial[OWN + half, rows] + from_core[buffer, half, rows]

    def combine(level, buffer, half):
        core_copy(buffer, half).wait_recv()
        steps, middle = code_scale(level)
        for step in (2, 1, 3):
            value = both_cores(buffer, half, (z_hi + step) % 4)
            code = jnp.round((jnp.log2(jnp.maximum(value, 2.0**-60)) - middle) * steps).astype(jnp.int32)
            codes[half, step - 1] = jnp.where(value > 0.0, code, ZERO_CODE).astype(jnp.int16)
            z_copy(buffer, half, step).start()

    def finish(level, buffer, half):
        steps, middle = code_scale(level)
        mine = both_cores(buffer, half, z_hi)
        for step in (1, 3, 2):
            z_copy(buffer, half, step).wait_recv()
            code = from_z[buffer, half, step - 1].astype(jnp.int32)
            value = jnp.exp2(code.astype(jnp.float32) * (1.0 / steps) + middle)
            mine = mine + jnp.where(code == ZERO_CODE, 0.0, value)
        raw = jnp.where(depth_ref[...] >= level, mine, 0.0)
        paths[level - 1, half * HALF : (half + 1) * HALF] = raw
        return raw

    def wait_sends():
        for half in range(2):
            core_copy(0, half).wait_send()
            for step in (1, 2, 3):
                z_copy(0, half, step).wait_send()

    def wait_tile_sends(buffer):
        sent = panel.at[buffer, pl.ds(0, SRCS - 1)]
        pltpu.make_async_copy(sent, sent, tile_send).wait()

    def reduce_level(level, buffer, out, block_product, drain, keep):
        with jax.named_scope("mm_last"):
            for half in range(2):
                partial[OTHER + half] = block_product(OTHER + half)
                core_copy(buffer, half).start()
                if half == 1:
                    with jax.named_scope("combine_0"):
                        combine(level, buffer, 0)
                partial[OWN + half] = block_product(OWN + half)
        with jax.named_scope("combine_1"):
            combine(level, buffer, 1)
            drain()
        squares = jnp.zeros((1, PANEL), jnp.float32)
        for half in range(2):
            with jax.named_scope("finish_%d" % half):
                raw = finish(level, buffer, half)
                squares = squares + jnp.sum(raw * raw, axis=0, keepdims=True)
                if out is not None:
                    panel[out, my_place, half * HALF : (half + 1) * HALF] = (raw * SHRINK).astype(jnp.bfloat16)
                    plane_start(out, half)
        keep(squares)

    mine_z = z_lo * N_COL + c
    mine_xy = x * 4 + y

    def z_peer(step):
        index = (mine_z + step) % 16
        return index, {"row": row_of(x, index // 8, y), "col": index % 8}

    def xy_peer(step):
        index = (mine_xy + step) % 16
        return index, {"row": row_of(index // 4, z_lo, index % 4), "col": c}

    def norm_start(which, source, slots, peer, mine):
        slots[mine] = source[...]

        @pl.loop(1, 16)
        def _(step):
            pltpu.make_async_remote_copy(
                src_ref=source,
                dst_ref=slots.at[mine],
                send_sem=norm_send.at[which],
                recv_sem=norm_recv.at[which, mine],
                device_id=peer(step)[1],
                device_id_type=MESH,
            ).start()

    def norm_wait(which, slots, peer):
        @pl.loop(1, 16)
        def _(step):
            slot = slots.at[peer(step)[0]]
            pltpu.make_async_copy(slot, slot, norm_recv.at[which, peer(step)[0]]).wait()

        sent = slots.at[pl.ds(0, 15)]
        pltpu.make_async_copy(sent, sent, norm_send.at[which]).wait()
        return jnp.sum(slots[...], axis=0)

    with jax.named_scope("onehot"):
        early[...] = jnp.zeros_like(early)

        @pl.loop(0, SRCS)
        def _(row):
            place = place_of(row // 8, (row // 4) % 2, row % 4)
            vertex = (row * N_COL + c) * TILE + lax.broadcasted_iota(jnp.int32, (TILE, PANEL), 0)
            panel[0, place] = (vertex == ids_ref[...]).astype(jnp.float32).astype(jnp.bfloat16)

    def first_product(block):
        partial[block] = product(0, [(0, j) for j in range(4)], block)

        @pl.loop(1, 3)
        def _(at_x):
            partial[block] += product(0, [(at_x, j) for j in range(4)], block)

        total = partial[block] + product(0, [(3, j) for j in range(4)], block)
        if block == OTHER:
            with jax.named_scope("barrier"):
                pl.semaphore_wait(barrier, N_ROW - 1 + 2 * (N_COL - 1))
        return total

    def keep_early(level):
        def keep(squares):
            early[pl.ds(level - 1, 1), :] = squares

        return keep

    reduce_level(1, 1, 1, first_product, lambda: None, keep_early(1))

    @pl.loop(2, LEVELS)
    def _(level):
        buffer = (level + 1) % 2
        chunks = gather(buffer, wait_sends)
        reduce_level(
            level,
            1 - buffer,
            1 - buffer,
            lambda block: partial[block] + product(buffer, chunks, block),
            lambda: wait_tile_sends(buffer),
            keep_early(level),
        )

    norm_start(0, early, early_z, z_peer, mine_z)
    buffer = (LEVELS + 1) % 2

    def middle_of_last():
        wait_sends()
        early[...] = norm_wait(0, early_z, z_peer)
        norm_start(1, early, early_xy, xy_peer, mine_xy)

    chunks = gather(buffer, middle_of_last)

    def keep_last(squares):
        last[...] = squares

    reduce_level(
        LEVELS,
        1 - buffer,
        None,
        lambda block: partial[block] + product(buffer, chunks, block),
        lambda: wait_tile_sends(buffer),
        keep_last,
    )

    with jax.named_scope("norm_z"):
        norm_start(2, last, last_z, z_peer, mine_z)
        wait_sends()
        totals = norm_wait(1, early_xy, xy_peer)
        last[...] = norm_wait(2, last_z, z_peer)
    with jax.named_scope("norm_xy"):
        norm_start(3, last, last_xy, xy_peer, mine_xy)
        last_total = norm_wait(3, last_xy, xy_peer)

    with jax.named_scope("outputs"):
        vertex = (r * N_COL + c) * TILE + lax.broadcasted_iota(jnp.int32, (TILE, PANEL), 0)
        sums = (vertex == ids_ref[...]).astype(jnp.float32)
        kappa = jnp.ones((1, PANEL), jnp.float32)
        for level in range(LEVELS):
            total = totals[level : level + 1] if level < LEVELS - 1 else last_total
            mean_square = total / VERTICES / kappa / kappa + EPSILON
            scale = kappa * jnp.sqrt(mean_square)
            sums = sums + paths[level] * (1.0 / scale)
            logs_ref[level : level + 1, :] = 0.5 * jnp.log(mean_square)
            kappa = scale * SHRINK
        sums_ref[...] = sums


def local(adj_tiles, tile_rows, tile_cols, tile_count, tile_depth, source_ids):
    hbm = pl.BlockSpec(memory_space=pltpu.HBM)
    vmem = pl.BlockSpec(memory_space=pltpu.VMEM)
    dense = pl.pallas_call(
        densify,
        out_shape=jax.ShapeDtypeStruct((DESTS * TILE, SRCS * TILE), jnp.bfloat16),
        in_specs=[hbm, hbm, hbm, hbm],
        out_specs=vmem,
        scratch_shapes=[
            pltpu.SMEM((1, 1), jnp.int32),
            pltpu.SMEM((1, 1, KMAX), jnp.int32),
            pltpu.SMEM((1, 1, KMAX), jnp.int32),
            pltpu.VMEM((KMAX, TILE, TILE), jnp.bfloat16),
            pltpu.SemaphoreType.DMA((3,)),
            pltpu.SemaphoreType.DMA((LOADS,)),
        ],
        compiler_params=pltpu.CompilerParams(vmem_limit_bytes=24 * 2**20),
        name="densify",
    )(tile_count, tile_rows, tile_cols, adj_tiles)
    return pl.pallas_call(
        levels_kernel,
        out_shape=(
            jax.ShapeDtypeStruct((TILE, PANEL), jnp.float32),
            jax.ShapeDtypeStruct((LEVELS, PANEL), jnp.float32),
        ),
        in_specs=[vmem, vmem, vmem],
        out_specs=(vmem, vmem),
        scratch_shapes=[
            pltpu.VMEM((2, SRCS, TILE, PANEL), jnp.bfloat16),
            pltpu.VMEM((4, BLOCK, PANEL), jnp.float32),
            pltpu.VMEM((2, 2, BLOCK, PANEL), jnp.float32),
            pltpu.VMEM((2, 3, HALF, PANEL), jnp.int16),
            pltpu.VMEM((2, 2, 3, HALF, PANEL), jnp.int16),
            pltpu.VMEM((LEVELS, TILE, PANEL), jnp.float32),
            pltpu.VMEM((8, PANEL), jnp.float32),
            pltpu.VMEM((16, 8, PANEL), jnp.float32),
            pltpu.VMEM((16, 8, PANEL), jnp.float32),
            pltpu.VMEM((1, PANEL), jnp.float32),
            pltpu.VMEM((16, 1, PANEL), jnp.float32),
            pltpu.VMEM((16, 1, PANEL), jnp.float32),
            pltpu.SemaphoreType.DMA,
            pltpu.SemaphoreType.DMA((2, 2, SRCS)),
            pltpu.SemaphoreType.DMA((2,)),
            pltpu.SemaphoreType.DMA((2, 2)),
            pltpu.SemaphoreType.DMA((2, 3)),
            pltpu.SemaphoreType.DMA((2, 2, 3)),
            pltpu.SemaphoreType.DMA((4,)),
            pltpu.SemaphoreType.DMA((4, 16)),
        ],
        compiler_params=pltpu.CompilerParams(
            collective_id=0, has_side_effects=True, vmem_limit_bytes=32 * 2**20
        ),
        name="levels",
    )(dense, tile_depth, source_ids.reshape(1, PANEL))


def solution(mesh):
    in_specs = (
        P("row", "col", None, None, None),
        P("row", "col", None),
        P("row", "col", None),
        P("row", "col"),
        P(("row", "col"), None),
        P(),
    )
    out_specs = (P(("row", "col"), None), P())
    return jax.shard_map(local, mesh=mesh, in_specs=in_specs, out_specs=out_specs, check_vma=False)
```

```python
import jax
import jax.numpy as jnp
from jax import lax
from jax.experimental import pallas as pl
from jax.experimental.pallas import tpu as pltpu
from jax.sharding import PartitionSpec as P

MESH = pl.DeviceIdType.MESH
TILE = 128
HALF = 64
PANEL = 128
LEVELS = 6
KMAX = 128
DESTS = 8
SRCS = 32
N_ROW = 32
N_COL = 8
VERTICES = 32768
EPSILON = 1e-06
SHRINK_BITS = 10
SHRINK = 2.0**-SHRINK_BITS
GROWTH_BITS = 17
CODES = 65000.0
ZERO_CODE = -32768
LOADS = 8
LOAD_SLOTS = KMAX // LOADS
TRIP = 4
BLOCK = 256
OTHER, OWN = 0, 2
PARTS = ((0, 48), (48, 48), (96, 32))
PLANE = ((0, 1), (1, 0), (3, 0), (1, 1), (3, 1), (2, 0), (2, 1))
FLAT = sorted(
    ((i, j) for i in range(4) for j in range(4) if i or j), key=lambda s: min(s[0], 4 - s[0]) + min(s[1], 4 - s[1])
)
NEAR = [(i, j) for i in (0, 1, 3) for j in (0, 1, 3)] + [(2, 0), (0, 2)]
FAR_ONE = [(2, 1), (1, 2)]
FAR_TWO = [(2, 3), (3, 2), (2, 2)]


def place_of(x, z_lo, y):
    return (x * 4 + y) * 2 + z_lo


def row_of(x, z_lo, y):
    return x * 8 + z_lo * 4 + y


def densify(count_hbm, rows_hbm, cols_hbm, tiles_hbm, dense_ref, count_ref, rows_ref, cols_ref, tiles, small_sem, load_sem):
    core = lax.axis_index("col") % 2

    def load(part):
        slots = pl.ds(part * LOAD_SLOTS, LOAD_SLOTS)
        return pltpu.make_async_copy(tiles_hbm.at[0, 0, slots], tiles.at[slots], load_sem.at[part])

    small = (
        pltpu.make_async_copy(count_hbm, count_ref, small_sem.at[0]),
        pltpu.make_async_copy(rows_hbm, rows_ref, small_sem.at[1]),
        pltpu.make_async_copy(cols_hbm, cols_ref, small_sem.at[2]),
    )
    for copy in small:
        copy.start()
    for part in range(LOADS):
        load(part).start()

    @pl.loop(0, DESTS * TILE // 16)
    def _(block):
        rows = pl.ds(pl.multiple_of(block * 16, 16), 16)
        dense_ref[rows, :] = jnp.zeros((16, SRCS * TILE), jnp.bfloat16)

    for copy in small:
        copy.wait()
    count = count_ref[0, 0]
    for part in range(LOADS):
        load(part).wait()
        first = part * (LOAD_SLOTS // TRIP)

        @pl.loop(first, jnp.minimum((count + TRIP - 1) // TRIP, first + LOAD_SLOTS // TRIP))
        def _(trip):
            for inner in range(TRIP):
                slot = trip * TRIP + inner
                dest = rows_ref[0, 0, slot]
                row = cols_ref[0, 0, slot]
                place = place_of(row // 8, (row // 4) % 2, row % 4)
                block = jnp.where(dest % 2 == core, OWN, OTHER)
                columns = pl.ds(pl.multiple_of(place * TILE, TILE), TILE)
                for half in range(2):
                    start = (block + half) * BLOCK + (dest // 2) * HALF
                    rows = pl.ds(pl.multiple_of(start, HALF), HALF)
                    tile = tiles[slot, half * HALF : (half + 1) * HALF]
                    dense_ref[rows, columns] += jnp.where(slot < count, tile, jnp.zeros_like(tile))


def levels_kernel(
    dense,
    depth_ref,
    ids_ref,
    sums_ref,
    logs_ref,
    panel,
    partial,
    from_core,
    codes,
    from_z,
    paths,
    early,
    early_z,
    early_xy,
    last,
    last_z,
    last_xy,
    tile_send,
    tile_recv,
    core_send,
    core_recv,
    z_send,
    z_recv,
    norm_send,
    norm_recv,
):
    r = lax.axis_index("row")
    c = lax.axis_index("col")
    x, z_lo, y = r // 8, (r // 4) % 2, r % 4
    z_hi, core = c // 2, c % 2
    my_place = place_of(x, z_lo, y)

    barrier = pltpu.get_barrier_semaphore()

    @pl.loop(1, N_ROW)
    def _(step):
        pl.semaphore_signal(
            barrier, inc=1, device_id={"row": (r + step) % N_ROW, "col": c}, device_id_type=MESH
        )

    @pl.loop(1, N_COL)
    def _(step):
        to = (c + step) % N_COL
        pl.semaphore_signal(barrier, inc=1, device_id={"row": r, "col": to}, device_id_type=MESH)
        pl.semaphore_signal(
            barrier, inc=1, device_id={"row": row_of(x, 1 - z_lo, y), "col": to}, device_id_type=MESH
        )

    def product(buffer, chunks, block):
        rows = slice(block * BLOCK, (block + 1) * BLOCK)
        total = None
        for at_x, at_y in chunks:
            index = at_x * 4 + at_y
            columns = pl.ds(pl.multiple_of(index * 2 * TILE, 2 * TILE), 2 * TILE)
            source = panel[buffer, pl.ds(index * 2, 2)].reshape(2 * TILE, PANEL)
            term = jnp.dot(dense[rows, columns], source, preferred_element_type=jnp.float32)
            total = term if total is None else total + term
        return total

    def part_of(buffer, place, part):
        start, size = PARTS[part]
        return panel.at[buffer, place, pl.ds(start, size)]

    def tile_copy(buffer, place, part, to_x, to_z, to_y):
        return pltpu.make_async_remote_copy(
            src_ref=part_of(buffer, place, part),
            dst_ref=part_of(buffer, place, part),
            send_sem=tile_send,
            recv_sem=tile_recv.at[buffer, part, place],
            device_id={"row": row_of(to_x, to_z, to_y), "col": c},
            device_id_type=MESH,
        )

    def wait_tile(buffer, place, part):
        ref = part_of(buffer, place, part)
        pltpu.make_async_copy(ref, ref, tile_recv.at[buffer, part, place]).wait()

    def at(part, along, across, z):
        ahead, side = ((x, y), (y, x))[part]
        ahead, side = (ahead + along) % 4, (side + across) % 4
        return (ahead, (z_lo + z) % 2, side) if part == 0 else (side, (z_lo + z) % 2, ahead)

    def flat(step_x, step_y, z):
        return (x + step_x) % 4, (z_lo + z) % 2, (y + step_y) % 4

    def send_along(buffer, place, part):
        for along in (1, 3, 2):
            tile_copy(buffer, place, part, *at(part, along, 0, 0)).start()

    def start_routed(buffer, part):
        for across, z in PLANE:
            tile_copy(buffer, my_place, part, *at(part, 0, across, z)).start()
        send_along(buffer, my_place, part)

    def start_flat(buffer):
        tile_copy(buffer, my_place, 2, *flat(0, 0, 1)).start()
        for step_x, step_y in FLAT:
            tile_copy(buffer, my_place, 2, *flat(step_x, step_y, 0)).start()

    def gather(buffer, wait_sends):
        with jax.named_scope("routed"):
            for across, z in PLANE:
                for part in range(2):
                    place = place_of(*at(part, 0, across, z))
                    wait_tile(buffer, place, part)
                    send_along(buffer, place, part)
        with jax.named_scope("flat"):
            for step_x, step_y in FLAT:
                place = place_of(*flat(step_x, step_y, 0))
                wait_tile(buffer, place, 2)
                tile_copy(buffer, place, 2, *flat(0, 0, 1)).start()
        with jax.named_scope("wait_near"):
            for z in range(2):
                for across in (0, 1, 3):
                    for along in (1, 3) if across else (1, 3, 2):
                        for part in range(2):
                            wait_tile(buffer, place_of(*at(part, along, across, z)), part)
            for step in NEAR:
                wait_tile(buffer, place_of(*flat(*step, 1)), 2)
        with jax.named_scope("mm_near"):
            wait_sends()
            chunks = [spot(*step) for step in NEAR]
            for block in range(4):
                partial[block] = product(buffer, chunks, block)
        with jax.named_scope("wait_one"):
            wait_far(buffer, FAR_ONE)
        with jax.named_scope("mm_one"):
            chunks = [spot(*step) for step in FAR_ONE]
            for block in range(4):
                partial[block] += product(buffer, chunks, block)
        with jax.named_scope("wait_two"):
            wait_far(buffer, FAR_TWO)
        return [spot(*step) for step in FAR_TWO]

    def spot(step_x, step_y):
        return (x + step_x) % 4, (y + step_y) % 4

    def wait_far(buffer, steps):
        for step_x, step_y in steps:
            for z in range(2):
                wait_tile(buffer, place_of(*at(0, step_x, step_y, z)), 0)
                wait_tile(buffer, place_of(*at(1, step_y, step_x, z)), 1)
            wait_tile(buffer, place_of(*flat(step_x, step_y, 1)), 2)

    def core_copy(buffer, half):
        return pltpu.make_async_remote_copy(
            src_ref=partial.at[OTHER + half],
            dst_ref=from_core.at[buffer, half],
            send_sem=core_send.at[half],
            recv_sem=core_recv.at[buffer, half],
            device_id={"row": r, "col": z_hi * 2 + 1 - core},
            device_id_type=MESH,
        )

    def z_copy(buffer, half, step):
        return pltpu.make_async_remote_copy(
            src_ref=codes.at[half, step - 1],
            dst_ref=from_z.at[buffer, half, step - 1],
            send_sem=z_send.at[half, step - 1],
            recv_sem=z_recv.at[buffer, half, step - 1],
            device_id={"row": r, "col": ((z_hi + step) % 4) * 2 + core},
            device_id_type=MESH,
        )

    def code_scale(level):
        before = (jnp.zeros((1, PANEL), jnp.int32) + (level - 1)).astype(jnp.float32)
        steps = CODES / (GROWTH_BITS * (before + 1.0) + 0.5)
        middle = 0.5 * (GROWTH_BITS + (GROWTH_BITS - 2 * SHRINK_BITS) * before)
        return steps, middle

    def both_cores(buffer, half, part):
        rows = pl.ds(pl.multiple_of(part * HALF, HALF), HALF)
        return partial[OWN + half, rows] + from_core[buffer, half, rows]

    def combine(level, buffer, half):
        core_copy(buffer, half).wait_recv()
        steps, middle = code_scale(level)
        for step in (2, 1, 3):
            value = both_cores(buffer, half, (z_hi + step) % 4)
            code = jnp.round((jnp.log2(jnp.maximum(value, 2.0**-60)) - middle) * steps).astype(jnp.int32)
            codes[half, step - 1] = jnp.where(value > 0.0, code, ZERO_CODE).astype(jnp.int16)
            z_copy(buffer, half, step).start()

    def finish(level, buffer, half):
        steps, middle = code_scale(level)
        mine = both_cores(buffer, half, z_hi)
        for step in (1, 3, 2):
            z_copy(buffer, half, step).wait_recv()
            code = from_z[buffer, half, step - 1].astype(jnp.int32)
            value = jnp.exp2(code.astype(jnp.float32) * (1.0 / steps) + middle)
            mine = mine + jnp.where(code == ZERO_CODE, 0.0, value)
        raw = jnp.where(depth_ref[...] >= level, mine, 0.0)
        paths[level - 1, half * HALF : (half + 1) * HALF] = raw
        return raw

    def wait_sends():
        for half in range(2):
            core_copy(0, half).wait_send()
            for step in (1, 2, 3):
                z_copy(0, half, step).wait_send()

    def wait_tile_sends(buffer):
        sent = panel.at[buffer, pl.ds(0, SRCS - 1)]
        pltpu.make_async_copy(sent, sent, tile_send).wait()

    def reduce_level(level, buffer, out, block_product, drain, keep):
        with jax.named_scope("mm_last"):
            for half in range(2):
                partial[OTHER + half] = block_product(OTHER + half)
                core_copy(buffer, half).start()
                if half == 1:
                    with jax.named_scope("combine_0"):
                        combine(level, buffer, 0)
                partial[OWN + half] = block_product(OWN + half)
        with jax.named_scope("combine_1"):
            combine(level, buffer, 1)
            drain()
        squares = jnp.zeros((1, PANEL), jnp.float32)
        for half in range(2):
            with jax.named_scope("finish_%d" % half):
                raw = finish(level, buffer, half)
                squares = squares + jnp.sum(raw * raw, axis=0, keepdims=True)
                if out is not None:
                    panel[out, my_place, half * HALF : (half + 1) * HALF] = (raw * SHRINK).astype(jnp.bfloat16)
                    start_routed(out, half)
                    if half == 1:
                        start_flat(out)
        keep(squares)

    mine_z = z_lo * N_COL + c
    mine_xy = x * 4 + y

    def z_peer(step):
        index = (mine_z + step) % 16
        return index, {"row": row_of(x, index // 8, y), "col": index % 8}

    def xy_peer(step):
        index = (mine_xy + step) % 16
        return index, {"row": row_of(index // 4, z_lo, index % 4), "col": c}

    def norm_start(which, source, slots, peer, mine):
        slots[mine] = source[...]

        @pl.loop(1, 16)
        def _(step):
            pltpu.make_async_remote_copy(
                src_ref=source,
                dst_ref=slots.at[mine],
                send_sem=norm_send.at[which],
                recv_sem=norm_recv.at[which, mine],
                device_id=peer(step)[1],
                device_id_type=MESH,
            ).start()

    def norm_wait(which, slots, peer):
        @pl.loop(1, 16)
        def _(step):
            slot = slots.at[peer(step)[0]]
            pltpu.make_async_copy(slot, slot, norm_recv.at[which, peer(step)[0]]).wait()

        sent = slots.at[pl.ds(0, 15)]
        pltpu.make_async_copy(sent, sent, norm_send.at[which]).wait()
        return jnp.sum(slots[...], axis=0)

    with jax.named_scope("onehot"):
        early[...] = jnp.zeros_like(early)

        @pl.loop(0, SRCS)
        def _(row):
            place = place_of(row // 8, (row // 4) % 2, row % 4)
            vertex = (row * N_COL + c) * TILE + lax.broadcasted_iota(jnp.int32, (TILE, PANEL), 0)
            panel[0, place] = (vertex == ids_ref[...]).astype(jnp.float32).astype(jnp.bfloat16)

    def first_product(block):
        partial[block] = product(0, [(0, j) for j in range(4)], block)

        @pl.loop(1, 3)
        def _(at_x):
            partial[block] += product(0, [(at_x, j) for j in range(4)], block)

        total = partial[block] + product(0, [(3, j) for j in range(4)], block)
        if block == OTHER:
            with jax.named_scope("barrier"):
                pl.semaphore_wait(barrier, N_ROW - 1 + 2 * (N_COL - 1))
        return total

    def keep_early(level):
        def keep(squares):
            early[pl.ds(level - 1, 1), :] = squares

        return keep

    reduce_level(1, 1, 1, first_product, lambda: None, keep_early(1))

    @pl.loop(2, LEVELS)
    def _(level):
        buffer = (level + 1) % 2
        chunks = gather(buffer, wait_sends)
        reduce_level(
            level,
            1 - buffer,
            1 - buffer,
            lambda block: partial[block] + product(buffer, chunks, block),
            lambda: wait_tile_sends(buffer),
            keep_early(level),
        )

    norm_start(0, early, early_z, z_peer, mine_z)
    buffer = (LEVELS + 1) % 2

    def middle_of_last():
        wait_sends()
        early[...] = norm_wait(0, early_z, z_peer)
        norm_start(1, early, early_xy, xy_peer, mine_xy)

    chunks = gather(buffer, middle_of_last)

    def keep_last(squares):
        last[...] = squares

    reduce_level(
        LEVELS,
        1 - buffer,
        None,
        lambda block: partial[block] + product(buffer, chunks, block),
        lambda: wait_tile_sends(buffer),
        keep_last,
    )

    with jax.named_scope("norm_z"):
        norm_start(2, last, last_z, z_peer, mine_z)
        wait_sends()
        totals = norm_wait(1, early_xy, xy_peer)
        last[...] = norm_wait(2, last_z, z_peer)
    with jax.named_scope("norm_xy"):
        norm_start(3, last, last_xy, xy_peer, mine_xy)
        last_total = norm_wait(3, last_xy, xy_peer)

    with jax.named_scope("outputs"):
        vertex = (r * N_COL + c) * TILE + lax.broadcasted_iota(jnp.int32, (TILE, PANEL), 0)
        sums = (vertex == ids_ref[...]).astype(jnp.float32)
        kappa = jnp.ones((1, PANEL), jnp.float32)
        for level in range(LEVELS):
            total = totals[level : level + 1] if level < LEVELS - 1 else last_total
            mean_square = total / VERTICES / kappa / kappa + EPSILON
            scale = kappa * jnp.sqrt(mean_square)
            sums = sums + paths[level] * (1.0 / scale)
            logs_ref[level : level + 1, :] = 0.5 * jnp.log(mean_square)
            kappa = scale * SHRINK
        sums_ref[...] = sums


def local(adj_tiles, tile_rows, tile_cols, tile_count, tile_depth, source_ids):
    hbm = pl.BlockSpec(memory_space=pltpu.HBM)
    vmem = pl.BlockSpec(memory_space=pltpu.VMEM)
    dense = pl.pallas_call(
        densify,
        out_shape=pltpu.VMEM((DESTS * TILE, SRCS * TILE), jnp.bfloat16),
        in_specs=[hbm, hbm, hbm, hbm],
        out_specs=vmem,
        scratch_shapes=[
            pltpu.SMEM((1, 1), jnp.int32),
            pltpu.SMEM((1, 1, KMAX), jnp.int32),
            pltpu.SMEM((1, 1, KMAX), jnp.int32),
            pltpu.VMEM((KMAX, TILE, TILE), jnp.bfloat16),
            pltpu.SemaphoreType.DMA((3,)),
            pltpu.SemaphoreType.DMA((LOADS,)),
        ],
        compiler_params=pltpu.CompilerParams(vmem_limit_bytes=53 * 2**20),
        name="densify",
    )(tile_count, tile_rows, tile_cols, adj_tiles)
    return pl.pallas_call(
        levels_kernel,
        out_shape=(
            jax.ShapeDtypeStruct((TILE, PANEL), jnp.float32),
            jax.ShapeDtypeStruct((LEVELS, PANEL), jnp.float32),
        ),
        in_specs=[vmem, vmem, vmem],
        out_specs=(vmem, vmem),
        scratch_shapes=[
            pltpu.VMEM((2, SRCS, TILE, PANEL), jnp.bfloat16),
            pltpu.VMEM((4, BLOCK, PANEL), jnp.float32),
            pltpu.VMEM((2, 2, BLOCK, PANEL), jnp.float32),
            pltpu.VMEM((2, 3, HALF, PANEL), jnp.int16),
            pltpu.VMEM((2, 2, 3, HALF, PANEL), jnp.int16),
            pltpu.VMEM((LEVELS, TILE, PANEL), jnp.float32),
            pltpu.VMEM((8, PANEL), jnp.float32),
            pltpu.VMEM((16, 8, PANEL), jnp.float32),
            pltpu.VMEM((16, 8, PANEL), jnp.float32),
            pltpu.VMEM((1, PANEL), jnp.float32),
            pltpu.VMEM((16, 1, PANEL), jnp.float32),
            pltpu.VMEM((16, 1, PANEL), jnp.float32),
            pltpu.SemaphoreType.DMA,
            pltpu.SemaphoreType.DMA((2, 3, SRCS)),
            pltpu.SemaphoreType.DMA((2,)),
            pltpu.SemaphoreType.DMA((2, 2)),
            pltpu.SemaphoreType.DMA((2, 3)),
            pltpu.SemaphoreType.DMA((2, 2, 3)),
            pltpu.SemaphoreType.DMA((4,)),
            pltpu.SemaphoreType.DMA((4, 16)),
        ],
        compiler_params=pltpu.CompilerParams(
            collective_id=0, has_side_effects=True, vmem_limit_bytes=32 * 2**20
        ),
        name="levels",
    )(dense, tile_depth, source_ids.reshape(1, PANEL))


def solution(mesh):
    in_specs = (
        P("row", "col", None, None, None),
        P("row", "col", None),
        P("row", "col", None),
        P("row", "col"),
        P(("row", "col"), None),
        P(),
    )
    out_specs = (P(("row", "col"), None), P())
    return jax.shard_map(local, mesh=mesh, in_specs=in_specs, out_specs=out_specs, check_vma=False)
```

```python
import jax
import jax.numpy as jnp
from jax import lax
from jax.experimental import pallas as pl
from jax.experimental.pallas import tpu as pltpu
from jax.sharding import PartitionSpec as P

MESH = pl.DeviceIdType.MESH
TILE = 128
HALF = 64
PANEL = 128
LEVELS = 6
KMAX = 128
DESTS = 8
SRCS = 32
N_ROW = 32
N_COL = 8
VERTICES = 32768
EPSILON = 1e-06
SHRINK_BITS = 10
SHRINK = 2.0**-SHRINK_BITS
GROWTH_BITS = 17
CODES = 65000.0
ZERO_CODE = -32768
LOADS = 8
LOAD_SLOTS = KMAX // LOADS
TRIP = 4
SIDE = 512
OTHER, OWN = 0, 1
PARTS = ((0, 48), (48, 48), (96, 32))
PLANE = ((0, 1), (1, 0), (3, 0), (1, 1), (3, 1), (2, 0), (2, 1))
FLAT = sorted(
    ((i, j) for i in range(4) for j in range(4) if i or j), key=lambda s: min(s[0], 4 - s[0]) + min(s[1], 4 - s[1])
)
GROUPS = (
    ((0, 0), (0, 1), (0, 3), (1, 0), (3, 0)),
    ((1, 1), (1, 3), (3, 1), (3, 3)),
    ((2, 0), (0, 2), (2, 1), (1, 2)),
    ((2, 3), (3, 2), (2, 2)),
)


def place_of(x, z_lo, y):
    return (x * 4 + y) * 2 + z_lo


def row_of(x, z_lo, y):
    return x * 8 + z_lo * 4 + y


def densify(count_hbm, rows_hbm, cols_hbm, tiles_hbm, dense_ref, count_ref, rows_ref, cols_ref, tiles, small_sem, load_sem):
    core = lax.axis_index("col") % 2

    def load(part):
        slots = pl.ds(part * LOAD_SLOTS, LOAD_SLOTS)
        return pltpu.make_async_copy(tiles_hbm.at[0, 0, slots], tiles.at[slots], load_sem.at[part])

    small = (
        pltpu.make_async_copy(count_hbm, count_ref, small_sem.at[0]),
        pltpu.make_async_copy(rows_hbm, rows_ref, small_sem.at[1]),
        pltpu.make_async_copy(cols_hbm, cols_ref, small_sem.at[2]),
    )
    for copy in small:
        copy.start()
    for part in range(LOADS):
        load(part).start()

    @pl.loop(0, SRCS * TILE // 64)
    def _(block):
        rows = pl.ds(pl.multiple_of(block * 64, 64), 64)
        dense_ref[rows, :] = jnp.zeros((64, DESTS * TILE), jnp.bfloat16)

    for copy in small:
        copy.wait()
    count = count_ref[0, 0]
    for part in range(LOADS):
        load(part).wait()
        first = part * (LOAD_SLOTS // TRIP)

        @pl.loop(first, jnp.minimum((count + TRIP - 1) // TRIP, first + LOAD_SLOTS // TRIP))
        def _(trip):
            for inner in range(TRIP):
                slot = trip * TRIP + inner
                dest = rows_ref[0, 0, slot]
                row = cols_ref[0, 0, slot]
                place = place_of(row // 8, (row // 4) % 2, row % 4)
                side = jnp.where(dest % 2 == core, OWN, OTHER)
                rows = pl.ds(pl.multiple_of(place * TILE, TILE), TILE)
                columns = pl.ds(pl.multiple_of(side * SIDE + (dest // 2) * TILE, TILE), TILE)
                tile = tiles[slot].T
                dense_ref[rows, columns] += jnp.where(slot < count, tile, jnp.zeros_like(tile))


def levels_kernel(
    dense,
    depth_ref,
    ids_ref,
    sums_ref,
    logs_ref,
    panel,
    depth,
    partial,
    from_core,
    codes,
    from_z,
    paths,
    early,
    early_z,
    early_xy,
    last,
    last_z,
    last_xy,
    tile_send,
    tile_recv,
    core_send,
    core_recv,
    z_send,
    z_recv,
    norm_send,
    norm_recv,
):
    r = lax.axis_index("row")
    c = lax.axis_index("col")
    x, z_lo, y = r // 8, (r // 4) % 2, r % 4
    z_hi, core = c // 2, c % 2
    my_place = place_of(x, z_lo, y)

    barrier = pltpu.get_barrier_semaphore()

    @pl.loop(1, N_ROW)
    def _(step):
        pl.semaphore_signal(
            barrier, inc=1, device_id={"row": (r + step) % N_ROW, "col": c}, device_id_type=MESH
        )

    @pl.loop(1, N_COL)
    def _(step):
        to = (c + step) % N_COL
        pl.semaphore_signal(barrier, inc=1, device_id={"row": r, "col": to}, device_id_type=MESH)
        pl.semaphore_signal(
            barrier, inc=1, device_id={"row": row_of(x, 1 - z_lo, y), "col": to}, device_id_type=MESH
        )

    def product(buffer, chunks, side):
        columns = slice(side * SIDE, (side + 1) * SIDE)
        total = None
        for at_x, at_y in chunks:
            index = at_x * 4 + at_y
            rows = pl.ds(pl.multiple_of(index * 2 * TILE, 2 * TILE), 2 * TILE)
            source = jnp.concatenate([panel[buffer, index * 2], panel[buffer, index * 2 + 1]], axis=1)
            term = jnp.dot(source, dense[rows, columns], preferred_element_type=jnp.float32)
            total = term if total is None else total + term
        return total

    def part_of(buffer, place, part):
        start, size = PARTS[part]
        return panel.at[buffer, place, pl.ds(start, size)]

    def tile_copy(buffer, place, part, to_x, to_z, to_y):
        return pltpu.make_async_remote_copy(
            src_ref=part_of(buffer, place, part),
            dst_ref=part_of(buffer, place, part),
            send_sem=tile_send,
            recv_sem=tile_recv.at[buffer, part, place],
            device_id={"row": row_of(to_x, to_z, to_y), "col": c},
            device_id_type=MESH,
        )

    def wait_tile(buffer, place, part):
        ref = part_of(buffer, place, part)
        pltpu.make_async_copy(ref, ref, tile_recv.at[buffer, part, place]).wait()

    def at(part, along, across, z):
        ahead, side = ((x, y), (y, x))[part]
        ahead, side = (ahead + along) % 4, (side + across) % 4
        return (ahead, (z_lo + z) % 2, side) if part == 0 else (side, (z_lo + z) % 2, ahead)

    def flat(step_x, step_y, z):
        return (x + step_x) % 4, (z_lo + z) % 2, (y + step_y) % 4

    def send_along(buffer, place, part):
        for along in (1, 3, 2):
            tile_copy(buffer, place, part, *at(part, along, 0, 0)).start()

    def start_routed(buffer, part):
        for across, z in PLANE:
            tile_copy(buffer, my_place, part, *at(part, 0, across, z)).start()
        send_along(buffer, my_place, part)

    def start_flat(buffer):
        tile_copy(buffer, my_place, 2, *flat(0, 0, 1)).start()
        for step_x, step_y in FLAT:
            tile_copy(buffer, my_place, 2, *flat(step_x, step_y, 0)).start()

    def gather(buffer, wait_sends):
        with jax.named_scope("routed"):
            for across, z in PLANE:
                for part in range(2):
                    place = place_of(*at(part, 0, across, z))
                    wait_tile(buffer, place, part)
                    send_along(buffer, place, part)
        with jax.named_scope("flat"):
            for step_x, step_y in FLAT:
                place = place_of(*flat(step_x, step_y, 0))
                wait_tile(buffer, place, 2)
                tile_copy(buffer, place, 2, *flat(0, 0, 1)).start()
        for number, group in enumerate(GROUPS):
            with jax.named_scope("wait_group_%d" % number):
                wait_group(buffer, group)
                if number == 0:
                    wait_sends()
            if number < len(GROUPS) - 1:
                with jax.named_scope("mm_group_%d" % number):
                    chunks = [spot(*step) for step in group]
                    for side in range(2):
                        if number == 0:
                            partial[side] = product(buffer, chunks, side)
                        else:
                            partial[side] += product(buffer, chunks, side)
        return [spot(*step) for step in GROUPS[-1]]

    def spot(step_x, step_y):
        return (x + step_x) % 4, (y + step_y) % 4

    def wait_group(buffer, steps):
        for step_x, step_y in steps:
            for z in range(2):
                if step_x:
                    wait_tile(buffer, place_of(*at(0, step_x, step_y, z)), 0)
                if step_y:
                    wait_tile(buffer, place_of(*at(1, step_y, step_x, z)), 1)
            wait_tile(buffer, place_of(*flat(step_x, step_y, 1)), 2)

    def core_copy(buffer, half):
        return pltpu.make_async_remote_copy(
            src_ref=partial.at[OTHER, pl.ds(half * HALF, HALF)],
            dst_ref=from_core.at[buffer, half],
            send_sem=core_send.at[half],
            recv_sem=core_recv.at[buffer, half],
            device_id={"row": r, "col": z_hi * 2 + 1 - core},
            device_id_type=MESH,
        )

    def z_copy(buffer, half, step):
        return pltpu.make_async_remote_copy(
            src_ref=codes.at[half, step - 1],
            dst_ref=from_z.at[buffer, half, step - 1],
            send_sem=z_send.at[half, step - 1],
            recv_sem=z_recv.at[buffer, half, step - 1],
            device_id={"row": r, "col": ((z_hi + step) % 4) * 2 + core},
            device_id_type=MESH,
        )

    def code_scale(level):
        before = (jnp.zeros((1, PANEL), jnp.int32) + (level - 1)).astype(jnp.float32)
        steps = CODES / (GROWTH_BITS * (before + 1.0) + 0.5)
        middle = 0.5 * (GROWTH_BITS + (GROWTH_BITS - 2 * SHRINK_BITS) * before)
        return steps, middle

    def both_cores(buffer, half, part):
        columns = pl.ds(pl.multiple_of(part * TILE, TILE), TILE)
        return partial[OWN, half * HALF : (half + 1) * HALF, columns] + from_core[buffer, half, :, columns]

    def combine(level, buffer, half):
        core_copy(buffer, half).wait_recv()
        steps, middle = code_scale(level)
        for step in (2, 1, 3):
            value = both_cores(buffer, half, (z_hi + step) % 4)
            code = jnp.round((jnp.log2(jnp.maximum(value, 2.0**-60)) - middle) * steps).astype(jnp.int32)
            codes[half, step - 1] = jnp.where(value > 0.0, code, ZERO_CODE).astype(jnp.int16)
            z_copy(buffer, half, step).start()

    def finish(level, buffer, half):
        steps, middle = code_scale(level)
        mine = both_cores(buffer, half, z_hi)
        for step in (1, 3, 2):
            z_copy(buffer, half, step).wait_recv()
            code = from_z[buffer, half, step - 1].astype(jnp.int32)
            value = jnp.exp2(code.astype(jnp.float32) * (1.0 / steps) + middle)
            mine = mine + jnp.where(code == ZERO_CODE, 0.0, value)
        rows = slice(half * HALF, (half + 1) * HALF)
        raw = jnp.where(depth[rows] >= level, mine, 0.0)
        paths[level - 1, rows] = raw
        return raw

    def wait_sends():
        for half in range(2):
            core_copy(0, half).wait_send()
            for step in (1, 2, 3):
                z_copy(0, half, step).wait_send()

    def wait_tile_sends(buffer):
        sent = panel.at[buffer, pl.ds(0, SRCS - 1)]
        pltpu.make_async_copy(sent, sent, tile_send).wait()

    def reduce_level(level, buffer, out, side_product, drain, keep):
        with jax.named_scope("mm_last"):
            partial[OTHER] = side_product(OTHER)
            for half in range(2):
                core_copy(buffer, half).start()
            partial[OWN] = side_product(OWN)
        with jax.named_scope("combine"):
            for half in range(2):
                combine(level, buffer, half)
            drain()
        for half in range(2):
            with jax.named_scope("finish_%d" % half):
                raw = finish(level, buffer, half)
                if out is not None:
                    panel[out, my_place, half * HALF : (half + 1) * HALF] = (raw * SHRINK).astype(jnp.bfloat16)
                    start_routed(out, half)
                    if half == 1:
                        start_flat(out)
        with jax.named_scope("squares"):
            by_vertex = paths[level - 1].T
            keep(jnp.sum(by_vertex * by_vertex, axis=0, keepdims=True))
            paths[level - 1] = by_vertex

    mine_z = z_lo * N_COL + c
    mine_xy = x * 4 + y

    def z_peer(step):
        index = (mine_z + step) % 16
        return index, {"row": row_of(x, index // 8, y), "col": index % 8}

    def xy_peer(step):
        index = (mine_xy + step) % 16
        return index, {"row": row_of(index // 4, z_lo, index % 4), "col": c}

    def norm_start(which, source, slots, peer, mine):
        slots[mine] = source[...]

        @pl.loop(1, 16)
        def _(step):
            pltpu.make_async_remote_copy(
                src_ref=source,
                dst_ref=slots.at[mine],
                send_sem=norm_send.at[which],
                recv_sem=norm_recv.at[which, mine],
                device_id=peer(step)[1],
                device_id_type=MESH,
            ).start()

    def norm_wait(which, slots, peer):
        @pl.loop(1, 16)
        def _(step):
            slot = slots.at[peer(step)[0]]
            pltpu.make_async_copy(slot, slot, norm_recv.at[which, peer(step)[0]]).wait()

        sent = slots.at[pl.ds(0, 15)]
        pltpu.make_async_copy(sent, sent, norm_send.at[which]).wait()
        return jnp.sum(slots[...], axis=0)

    with jax.named_scope("onehot"):
        early[...] = jnp.zeros_like(early)
        depth[...] = jnp.broadcast_to(depth_ref[...], (TILE, PANEL)).astype(jnp.float32).T.astype(jnp.int32)
        ids = jnp.broadcast_to(ids_ref[...], (TILE, PANEL)).astype(jnp.float32).T.astype(jnp.int32)

        @pl.loop(0, SRCS)
        def _(row):
            place = place_of(row // 8, (row // 4) % 2, row % 4)
            vertex = (row * N_COL + c) * TILE + lax.broadcasted_iota(jnp.int32, (PANEL, TILE), 1)
            panel[0, place] = (vertex == ids).astype(jnp.float32).astype(jnp.bfloat16)

    def first_product(side):
        partial[side] = product(0, [(0, j) for j in range(4)], side)

        @pl.loop(1, 3)
        def _(at_x):
            partial[side] += product(0, [(at_x, j) for j in range(4)], side)

        total = partial[side] + product(0, [(3, j) for j in range(4)], side)
        if side == OTHER:
            with jax.named_scope("barrier"):
                pl.semaphore_wait(barrier, N_ROW - 1 + 2 * (N_COL - 1))
        return total

    def keep_early(level):
        def keep(squares):
            early[pl.ds(level - 1, 1), :] = squares

        return keep

    reduce_level(1, 1, 1, first_product, lambda: None, keep_early(1))

    @pl.loop(2, LEVELS)
    def _(level):
        buffer = (level + 1) % 2
        chunks = gather(buffer, wait_sends)
        reduce_level(
            level,
            1 - buffer,
            1 - buffer,
            lambda side: partial[side] + product(buffer, chunks, side),
            lambda: wait_tile_sends(buffer),
            keep_early(level),
        )

    norm_start(0, early, early_z, z_peer, mine_z)
    buffer = (LEVELS + 1) % 2

    def middle_of_last():
        wait_sends()
        early[...] = norm_wait(0, early_z, z_peer)
        norm_start(1, early, early_xy, xy_peer, mine_xy)

    chunks = gather(buffer, middle_of_last)

    def keep_last(squares):
        last[...] = squares

    reduce_level(
        LEVELS,
        1 - buffer,
        None,
        lambda side: partial[side] + product(buffer, chunks, side),
        lambda: wait_tile_sends(buffer),
        keep_last,
    )

    with jax.named_scope("norm_z"):
        norm_start(2, last, last_z, z_peer, mine_z)
        wait_sends()
        totals = norm_wait(1, early_xy, xy_peer)
        last[...] = norm_wait(2, last_z, z_peer)
    with jax.named_scope("norm_xy"):
        norm_start(3, last, last_xy, xy_peer, mine_xy)
        last_total = norm_wait(3, last_xy, xy_peer)

    with jax.named_scope("outputs"):
        vertex = (r * N_COL + c) * TILE + lax.broadcasted_iota(jnp.int32, (TILE, PANEL), 0)
        sums = (vertex == ids_ref[...]).astype(jnp.float32)
        kappa = jnp.ones((1, PANEL), jnp.float32)
        for level in range(LEVELS):
            total = totals[level : level + 1] if level < LEVELS - 1 else last_total
            mean_square = total / VERTICES / kappa / kappa + EPSILON
            scale = kappa * jnp.sqrt(mean_square)
            sums = sums + paths[level] * (1.0 / scale)
            logs_ref[level : level + 1, :] = 0.5 * jnp.log(mean_square)
            kappa = scale * SHRINK
        sums_ref[...] = sums


def local(adj_tiles, tile_rows, tile_cols, tile_count, tile_depth, source_ids):
    hbm = pl.BlockSpec(memory_space=pltpu.HBM)
    vmem = pl.BlockSpec(memory_space=pltpu.VMEM)
    dense = pl.pallas_call(
        densify,
        out_shape=pltpu.VMEM((SRCS * TILE, DESTS * TILE), jnp.bfloat16),
        in_specs=[hbm, hbm, hbm, hbm],
        out_specs=vmem,
        scratch_shapes=[
            pltpu.SMEM((1, 1), jnp.int32),
            pltpu.SMEM((1, 1, KMAX), jnp.int32),
            pltpu.SMEM((1, 1, KMAX), jnp.int32),
            pltpu.VMEM((KMAX, TILE, TILE), jnp.bfloat16),
            pltpu.SemaphoreType.DMA((3,)),
            pltpu.SemaphoreType.DMA((LOADS,)),
        ],
        compiler_params=pltpu.CompilerParams(vmem_limit_bytes=53 * 2**20),
        name="densify",
    )(tile_count, tile_rows, tile_cols, adj_tiles)
    return pl.pallas_call(
        levels_kernel,
        out_shape=(
            jax.ShapeDtypeStruct((TILE, PANEL), jnp.float32),
            jax.ShapeDtypeStruct((LEVELS, PANEL), jnp.float32),
        ),
        in_specs=[vmem, vmem, vmem],
        out_specs=(vmem, vmem),
        scratch_shapes=[
            pltpu.VMEM((2, SRCS, TILE, PANEL), jnp.bfloat16),
            pltpu.VMEM((PANEL, TILE), jnp.int32),
            pltpu.VMEM((2, PANEL, SIDE), jnp.float32),
            pltpu.VMEM((2, 2, HALF, SIDE), jnp.float32),
            pltpu.VMEM((2, 3, HALF, PANEL), jnp.int16),
            pltpu.VMEM((2, 2, 3, HALF, PANEL), jnp.int16),
            pltpu.VMEM((LEVELS, TILE, PANEL), jnp.float32),
            pltpu.VMEM((8, PANEL), jnp.float32),
            pltpu.VMEM((16, 8, PANEL), jnp.float32),
            pltpu.VMEM((16, 8, PANEL), jnp.float32),
            pltpu.VMEM((1, PANEL), jnp.float32),
            pltpu.VMEM((16, 1, PANEL), jnp.float32),
            pltpu.VMEM((16, 1, PANEL), jnp.float32),
            pltpu.SemaphoreType.DMA,
            pltpu.SemaphoreType.DMA((2, 3, SRCS)),
            pltpu.SemaphoreType.DMA((2,)),
            pltpu.SemaphoreType.DMA((2, 2)),
            pltpu.SemaphoreType.DMA((2, 3)),
            pltpu.SemaphoreType.DMA((2, 2, 3)),
            pltpu.SemaphoreType.DMA((4,)),
            pltpu.SemaphoreType.DMA((4, 16)),
        ],
        compiler_params=pltpu.CompilerParams(
            collective_id=0, has_side_effects=True, vmem_limit_bytes=32 * 2**20
        ),
        name="levels",
    )(dense, tile_depth, source_ids.reshape(1, PANEL))


def solution(mesh):
    in_specs = (
        P("row", "col", None, None, None),
        P("row", "col", None),
        P("row", "col", None),
        P("row", "col"),
        P(("row", "col"), None),
        P(),
    )
    out_specs = (P(("row", "col"), None), P())
    return jax.shard_map(local, mesh=mesh, in_specs=in_specs, out_specs=out_specs, check_vma=False)
```

```python
import jax
import jax.numpy as jnp
from jax import lax
from jax.experimental import pallas as pl
from jax.experimental.pallas import tpu as pltpu
from jax.sharding import PartitionSpec as P

MESH = pl.DeviceIdType.MESH
TILE = 128
HALF = 64
PANEL = 128
LEVELS = 6
KMAX = 128
DESTS = 8
SRCS = 32
N_ROW = 32
N_COL = 8
VERTICES = 32768
EPSILON = 1e-06
SHRINK_BITS = 10
SHRINK = 2.0**-SHRINK_BITS
GROWTH_BITS = 17
CODES = 65000.0
ZERO_CODE = -32768
LOADS = 8
LOAD_SLOTS = KMAX // LOADS
TRIP = 16
SIDE = 512
OTHER, OWN = 0, 1
PARTS = ((0, 48), (48, 48), (96, 32))
PLANE = ((0, 1), (1, 0), (3, 0), (1, 1), (3, 1), (2, 0), (2, 1))
FLAT = sorted(
    ((i, j) for i in range(4) for j in range(4) if i or j), key=lambda s: min(s[0], 4 - s[0]) + min(s[1], 4 - s[1])
)
RELAYS = (
    *((0, i, z) for i, z in ((0, 1), (1, 0), (3, 0), (1, 1), (3, 1))),
    *((1, i, z) for i, z in ((0, 1), (1, 0), (3, 0))),
    *((0, i, z) for i, z in ((2, 0), (2, 1))),
    *((1, i, z) for i, z in ((1, 1), (3, 1), (2, 0), (2, 1))),
)
GROUPS = (
    ((0, 0), (0, 1), (0, 3), (1, 0), (3, 0)),
    ((1, 1), (1, 3), (3, 1), (3, 3)),
    ((2, 0), (0, 2), (2, 1), (1, 2)),
    ((2, 3), (3, 2), (2, 2)),
)


def place_of(step_x, step_y, step_z):
    return (step_x % 4 * 4 + step_y % 4) * 2 + step_z % 2


def row_of(x, z_lo, y):
    return x * 8 + z_lo * 4 + y


def densify(count_hbm, rows_hbm, cols_hbm, tiles_hbm, dense_ref, count_ref, rows_ref, cols_ref, tiles, small_sem, load_sem):
    core = lax.axis_index("col") % 2
    r = lax.axis_index("row")
    x, z_lo, y = r // 8, (r // 4) % 2, r % 4

    def load(part):
        slots = pl.ds(part * LOAD_SLOTS, LOAD_SLOTS)
        return pltpu.make_async_copy(tiles_hbm.at[0, 0, slots], tiles.at[slots], load_sem.at[part])

    small = (
        pltpu.make_async_copy(count_hbm, count_ref, small_sem.at[0]),
        pltpu.make_async_copy(rows_hbm, rows_ref, small_sem.at[1]),
        pltpu.make_async_copy(cols_hbm, cols_ref, small_sem.at[2]),
    )
    for copy in small:
        copy.start()
    for part in range(LOADS):
        load(part).start()

    @pl.loop(0, SRCS * TILE // 64)
    def _(block):
        rows = pl.ds(pl.multiple_of(block * 64, 64), 64)
        dense_ref[rows, :] = jnp.zeros((64, DESTS * TILE), jnp.bfloat16)

    for copy in small:
        copy.wait()
    count = count_ref[0, 0]
    for part in range(LOADS):
        load(part).wait()
        first = part * (LOAD_SLOTS // TRIP)

        @pl.loop(first, jnp.minimum((count + TRIP - 1) // TRIP, first + LOAD_SLOTS // TRIP))
        def _(trip):
            for inner in range(TRIP):
                slot = trip * TRIP + inner
                dest = rows_ref[0, 0, slot]
                row = cols_ref[0, 0, slot]
                steps = (((row >> 3) - x) & 3, (row - y) & 3, ((row >> 2) ^ z_lo) & 1)
                place = steps[0] * 8 + steps[1] * 2 + steps[2]
                side = 1 - ((dest ^ core) & 1)
                rows = pl.ds(pl.multiple_of(place * TILE, TILE), TILE)
                columns = pl.ds(pl.multiple_of(side * SIDE + (dest >> 1) * TILE, TILE), TILE)
                tile = tiles[slot].T
                dense_ref[rows, columns] += jnp.where(slot < count, tile, jnp.zeros_like(tile))


def levels_kernel(
    dense,
    depth_ref,
    ids_ref,
    sums_ref,
    logs_ref,
    panel,
    depth,
    partial,
    from_core,
    codes,
    from_z,
    paths,
    early,
    early_z,
    early_xy,
    last,
    last_z,
    last_xy,
    tile_send,
    tile_recv,
    core_send,
    core_recv,
    z_send,
    z_recv,
    norm_send,
    norm_recv,
):
    r = lax.axis_index("row")
    c = lax.axis_index("col")
    x, z_lo, y = r // 8, (r // 4) % 2, r % 4
    z_hi, core = c // 2, c % 2

    barrier = pltpu.get_barrier_semaphore()

    @pl.loop(1, N_ROW)
    def _(step):
        pl.semaphore_signal(
            barrier, inc=1, device_id={"row": (r + step) % N_ROW, "col": c}, device_id_type=MESH
        )

    @pl.loop(1, N_COL)
    def _(step):
        to = (c + step) % N_COL
        pl.semaphore_signal(barrier, inc=1, device_id={"row": r, "col": to}, device_id_type=MESH)
        pl.semaphore_signal(
            barrier, inc=1, device_id={"row": row_of(x, 1 - z_lo, y), "col": to}, device_id_type=MESH
        )

    def product(tiles, chunks, side):
        columns = slice(side * SIDE, (side + 1) * SIDE)
        total = None
        for step_x, step_y in chunks:
            index = step_x * 4 + step_y
            rows = slice(index * 2 * TILE, (index + 1) * 2 * TILE)
            source = jnp.concatenate([tiles[index * 2], tiles[index * 2 + 1]], axis=1)
            term = jnp.dot(source, dense[rows, columns], preferred_element_type=jnp.float32)
            total = term if total is None else total + term
        return total

    def part_of(buffer, place, part):
        start, size = PARTS[part]
        return panel.at[buffer, place, pl.ds(start, size)]

    def tile_copy(buffer, part, tile, to):
        there = place_of(*(i - j for i, j in zip(tile, to)))
        return pltpu.make_async_remote_copy(
            src_ref=part_of(buffer, place_of(*tile), part),
            dst_ref=part_of(buffer, there, part),
            send_sem=tile_send,
            recv_sem=tile_recv.at[buffer, part, there],
            device_id={"row": row_of((x + to[0]) % 4, (z_lo + to[2]) % 2, (y + to[1]) % 4), "col": c},
            device_id_type=MESH,
        )

    def wait_tile(buffer, part, tile):
        ref = part_of(buffer, place_of(*tile), part)
        pltpu.make_async_copy(ref, ref, tile_recv.at[buffer, part, place_of(*tile)]).wait()

    def at(part, along, across, z):
        return (along, across, z) if part == 0 else (across, along, z)

    def send_along(buffer, part, tile):
        for along in (1, 3, 2):
            tile_copy(buffer, part, tile, at(part, along, 0, 0)).start()

    def start_routed(buffer, part):
        for across, z in PLANE:
            tile_copy(buffer, part, (0, 0, 0), at(part, 0, across, z)).start()
        send_along(buffer, part, (0, 0, 0))

    def start_flat(buffer):
        tile_copy(buffer, 2, (0, 0, 0), (0, 0, 1)).start()
        for step in FLAT:
            tile_copy(buffer, 2, (0, 0, 0), (*step, 0)).start()

    def gather(buffer, wait_sends):
        with jax.named_scope("routed"):
            for part, across, z in RELAYS:
                wait_tile(buffer, part, at(part, 0, across, z))
                send_along(buffer, part, at(part, 0, across, z))
        with jax.named_scope("flat"):
            for step in FLAT:
                wait_tile(buffer, 2, (*step, 0))
                tile_copy(buffer, 2, (*step, 0), (0, 0, 1)).start()
        for number, group in enumerate(GROUPS):
            with jax.named_scope("wait_group_%d" % number):
                wait_group(buffer, group)
                if number == 0:
                    wait_sends()
            if number < len(GROUPS) - 1:
                with jax.named_scope("mm_group_%d" % number):
                    for side in range(2):
                        if number == 0:
                            partial[side] = product(panel.at[buffer], group, side)
                        else:
                            partial[side] += product(panel.at[buffer], group, side)

    def wait_group(buffer, steps):
        for step in steps:
            for z in range(2):
                if step[0]:
                    wait_tile(buffer, 0, (*step, z))
                if step[1]:
                    wait_tile(buffer, 1, (*step, z))
            wait_tile(buffer, 2, (*step, 1))

    def core_copy(buffer, half, part):
        columns = pl.ds(pl.multiple_of(part * TILE, TILE), TILE)
        return pltpu.make_async_remote_copy(
            src_ref=partial.at[OTHER, pl.ds(half * HALF, HALF), columns],
            dst_ref=from_core.at[buffer, half, part],
            send_sem=core_send.at[half, part],
            recv_sem=core_recv.at[buffer, half, part],
            device_id={"row": r, "col": z_hi * 2 + 1 - core},
            device_id_type=MESH,
        )

    def z_copy(buffer, half, step):
        return pltpu.make_async_remote_copy(
            src_ref=codes.at[half, step - 1],
            dst_ref=from_z.at[buffer, half, step - 1],
            send_sem=z_send.at[half, step - 1],
            recv_sem=z_recv.at[buffer, half, step - 1],
            device_id={"row": r, "col": ((z_hi + step) % 4) * 2 + core},
            device_id_type=MESH,
        )

    def code_scale(level):
        before = (jnp.zeros((1, PANEL), jnp.int32) + (level - 1)).astype(jnp.float32)
        steps = CODES / (GROWTH_BITS * (before + 1.0) + 0.5)
        middle = 0.5 * (GROWTH_BITS + (GROWTH_BITS - 2 * SHRINK_BITS) * before)
        return steps, middle

    def both_cores(buffer, half, part):
        core_copy(buffer, half, part).wait_recv()
        columns = pl.ds(pl.multiple_of(part * TILE, TILE), TILE)
        return partial[OWN, half * HALF : (half + 1) * HALF, columns] + from_core[buffer, half, part]

    def combine(level, buffer, half):
        steps, middle = code_scale(level)
        for step in (2, 1, 3):
            value = both_cores(buffer, half, (z_hi + step) % 4)
            code = jnp.round((jnp.log2(jnp.maximum(value, 2.0**-60)) - middle) * steps).astype(jnp.int32)
            codes[half, step - 1] = jnp.where(value > 0.0, code, ZERO_CODE).astype(jnp.int16)
            z_copy(buffer, half, step).start()

    def finish(level, buffer, half):
        steps, middle = code_scale(level)
        mine = both_cores(buffer, half, z_hi)
        for step in (1, 3, 2):
            z_copy(buffer, half, step).wait_recv()
            code = from_z[buffer, half, step - 1].astype(jnp.int32)
            value = jnp.exp2(code.astype(jnp.float32) * (1.0 / steps) + middle)
            mine = mine + jnp.where(code == ZERO_CODE, 0.0, value)
        rows = slice(half * HALF, (half + 1) * HALF)
        raw = jnp.where(depth[rows] >= level, mine, 0.0)
        paths[level - 1, rows] = raw
        return raw

    def wait_sends():
        for half in range(2):
            for part in range(4):
                core_copy(0, half, part).wait_send()
            for step in (1, 2, 3):
                z_copy(0, half, step).wait_send()

    def wait_tile_sends(buffer):
        sent = panel.at[buffer, pl.ds(0, SRCS - 1)]
        pltpu.make_async_copy(sent, sent, tile_send).wait()

    def reduce_level(level, buffer, out, side_product, drain, keep, early_core):
        def other_side():
            partial[OTHER] = side_product(OTHER)
            for half in range(2):
                for step in (2, 1, 3, 0):
                    core_copy(buffer, half, (z_hi + step) % 4).start()

        def own_side():
            partial[OWN] = side_product(OWN)

        def combine_both():
            for half in range(2):
                combine(level, buffer, half)

        def own_first():
            own_side()
            combine_both()
            other_side()

        def other_first():
            other_side()
            own_side()
            combine_both()

        with jax.named_scope("mm_last"):
            if early_core is None:
                other_first()
            else:
                pl.when(core == early_core)(other_first)
                pl.when(core != early_core)(own_first)
            drain()
        for half in range(2):
            with jax.named_scope("finish_%d" % half):
                raw = finish(level, buffer, half)
                if out is not None:
                    panel[out, 0, half * HALF : (half + 1) * HALF] = (raw * SHRINK).astype(jnp.bfloat16)
                    start_routed(out, half)
                    if half == 1:
                        start_flat(out)
        with jax.named_scope("squares"):
            by_vertex = paths[level - 1].T
            keep(jnp.sum(by_vertex * by_vertex, axis=0, keepdims=True))
            paths[level - 1] = by_vertex

    mine_z = z_lo * N_COL + c
    mine_xy = x * 4 + y

    def z_peer(step):
        index = (mine_z + step) % 16
        return index, {"row": row_of(x, index // 8, y), "col": index % 8}

    def xy_peer(step):
        index = (mine_xy + step) % 16
        return index, {"row": row_of(index // 4, z_lo, index % 4), "col": c}

    def norm_start(which, source, slots, peer, mine):
        slots[mine] = source[...]

        @pl.loop(1, 16)
        def _(step):
            pltpu.make_async_remote_copy(
                src_ref=source,
                dst_ref=slots.at[mine],
                send_sem=norm_send.at[which],
                recv_sem=norm_recv.at[which, mine],
                device_id=peer(step)[1],
                device_id_type=MESH,
            ).start()

    def norm_wait(which, slots, peer):
        @pl.loop(1, 16)
        def _(step):
            slot = slots.at[peer(step)[0]]
            pltpu.make_async_copy(slot, slot, norm_recv.at[which, peer(step)[0]]).wait()

        sent = slots.at[pl.ds(0, 15)]
        pltpu.make_async_copy(sent, sent, norm_send.at[which]).wait()
        return jnp.sum(slots[...], axis=0)

    with jax.named_scope("onehot"):
        early[...] = jnp.zeros_like(early)
        depth[...] = jnp.broadcast_to(depth_ref[...], (TILE, PANEL)).astype(jnp.float32).T.astype(jnp.int32)
        ids = jnp.broadcast_to(ids_ref[...], (TILE, PANEL)).astype(jnp.float32).T.astype(jnp.int32)
        offsets = ids - lax.broadcasted_iota(jnp.int32, (PANEL, TILE), 1)

        @pl.loop(0, SRCS // 4)
        def _(quad):
            for inner in range(4):
                step_x, step_y = quad // 2, quad % 2 * 2 + inner // 2
                row = row_of((x + step_x) % 4, (z_lo + inner) % 2, (y + step_y) % 4)
                hit = offsets == (row * N_COL + c) * TILE
                panel[0, quad * 4 + inner] = hit.astype(jnp.float32).astype(jnp.bfloat16)

    def first_product(side):
        total = product(panel.at[0], [(i, j) for i in range(4) for j in range(4)], side)
        if side == OTHER:
            with jax.named_scope("barrier"):
                pl.semaphore_wait(barrier, N_ROW - 1 + 2 * (N_COL - 1))
        return total

    def keep_early(level):
        def keep(squares):
            early[pl.ds(level - 1, 1), :] = squares

        return keep

    reduce_level(1, 1, 1, first_product, lambda: None, keep_early(1), None)

    @pl.loop(2, LEVELS)
    def _(level):
        buffer = (level + 1) % 2
        gather(buffer, wait_sends)
        reduce_level(
            level,
            1 - buffer,
            1 - buffer,
            lambda side: partial[side] + product(panel.at[buffer], GROUPS[-1], side),
            lambda: wait_tile_sends(buffer),
            keep_early(level),
            1,
        )

    norm_start(0, early, early_z, z_peer, mine_z)
    buffer = (LEVELS + 1) % 2

    def middle_of_last():
        wait_sends()
        early[...] = norm_wait(0, early_z, z_peer)
        norm_start(1, early, early_xy, xy_peer, mine_xy)

    gather(buffer, middle_of_last)

    def keep_last(squares):
        last[...] = squares

    reduce_level(
        LEVELS,
        1 - buffer,
        None,
        lambda side: partial[side] + product(panel.at[buffer], GROUPS[-1], side),
        lambda: wait_tile_sends(buffer),
        keep_last,
        1,
    )

    with jax.named_scope("norm_z"):
        norm_start(2, last, last_z, z_peer, mine_z)
        wait_sends()
        totals = norm_wait(1, early_xy, xy_peer)
        last[...] = norm_wait(2, last_z, z_peer)
    with jax.named_scope("norm_xy"):
        norm_start(3, last, last_xy, xy_peer, mine_xy)
        last_total = norm_wait(3, last_xy, xy_peer)

    with jax.named_scope("outputs"):
        vertex = (r * N_COL + c) * TILE + lax.broadcasted_iota(jnp.int32, (TILE, PANEL), 0)
        sums = (vertex == ids_ref[...]).astype(jnp.float32)
        kappa = jnp.ones((1, PANEL), jnp.float32)
        for level in range(LEVELS):
            total = totals[level : level + 1] if level < LEVELS - 1 else last_total
            mean_square = total / VERTICES / kappa / kappa + EPSILON
            scale = kappa * jnp.sqrt(mean_square)
            sums = sums + paths[level] * (1.0 / scale)
            logs_ref[level : level + 1, :] = 0.5 * jnp.log(mean_square)
            kappa = scale * SHRINK
        sums_ref[...] = sums


def local(adj_tiles, tile_rows, tile_cols, tile_count, tile_depth, source_ids):
    hbm = pl.BlockSpec(memory_space=pltpu.HBM)
    vmem = pl.BlockSpec(memory_space=pltpu.VMEM)
    dense = pl.pallas_call(
        densify,
        out_shape=pltpu.VMEM((SRCS * TILE, DESTS * TILE), jnp.bfloat16),
        in_specs=[hbm, hbm, hbm, hbm],
        out_specs=vmem,
        scratch_shapes=[
            pltpu.SMEM((1, 1), jnp.int32),
            pltpu.SMEM((1, 1, KMAX), jnp.int32),
            pltpu.SMEM((1, 1, KMAX), jnp.int32),
            pltpu.VMEM((KMAX, TILE, TILE), jnp.bfloat16),
            pltpu.SemaphoreType.DMA((3,)),
            pltpu.SemaphoreType.DMA((LOADS,)),
        ],
        compiler_params=pltpu.CompilerParams(vmem_limit_bytes=53 * 2**20),
        name="densify",
    )(tile_count, tile_rows, tile_cols, adj_tiles)
    return pl.pallas_call(
        levels_kernel,
        out_shape=(
            jax.ShapeDtypeStruct((TILE, PANEL), jnp.float32),
            jax.ShapeDtypeStruct((LEVELS, PANEL), jnp.float32),
        ),
        in_specs=[vmem, vmem, vmem],
        out_specs=(vmem, vmem),
        scratch_shapes=[
            pltpu.VMEM((2, SRCS, TILE, PANEL), jnp.bfloat16),
            pltpu.VMEM((PANEL, TILE), jnp.int32),
            pltpu.VMEM((2, PANEL, SIDE), jnp.float32),
            pltpu.VMEM((2, 2, 4, HALF, TILE), jnp.float32),
            pltpu.VMEM((2, 3, HALF, PANEL), jnp.int16),
            pltpu.VMEM((2, 2, 3, HALF, PANEL), jnp.int16),
            pltpu.VMEM((LEVELS, TILE, PANEL), jnp.float32),
            pltpu.VMEM((8, PANEL), jnp.float32),
            pltpu.VMEM((16, 8, PANEL), jnp.float32),
            pltpu.VMEM((16, 8, PANEL), jnp.float32),
            pltpu.VMEM((1, PANEL), jnp.float32),
            pltpu.VMEM((16, 1, PANEL), jnp.float32),
            pltpu.VMEM((16, 1, PANEL), jnp.float32),
            pltpu.SemaphoreType.DMA,
            pltpu.SemaphoreType.DMA((2, 3, SRCS)),
            pltpu.SemaphoreType.DMA((2, 4)),
            pltpu.SemaphoreType.DMA((2, 2, 4)),
            pltpu.SemaphoreType.DMA((2, 3)),
            pltpu.SemaphoreType.DMA((2, 2, 3)),
            pltpu.SemaphoreType.DMA((4,)),
            pltpu.SemaphoreType.DMA((4, 16)),
        ],
        compiler_params=pltpu.CompilerParams(
            collective_id=0, has_side_effects=True, vmem_limit_bytes=32 * 2**20
        ),
        name="levels",
    )(dense, tile_depth, source_ids.reshape(1, PANEL))


def solution(mesh):
    in_specs = (
        P("row", "col", None, None, None),
        P("row", "col", None),
        P("row", "col", None),
        P("row", "col"),
        P(("row", "col"), None),
        P(),
    )
    out_specs = (P(("row", "col"), None), P())
    return jax.shard_map(local, mesh=mesh, in_specs=in_specs, out_specs=out_specs, check_vma=False)
```

```python
import jax
import jax.numpy as jnp
from jax import lax
from jax.experimental import pallas as pl
from jax.experimental.pallas import tpu as pltpu
from jax.sharding import PartitionSpec as P

MESH = pl.DeviceIdType.MESH
TILE = 128
PIECES = ((0, 48), (48, 80))
LONGEST = 80
PANEL = 128
LEVELS = 6
KMAX = 128
DESTS = 8
SRCS = 32
N_ROW = 32
N_COL = 8
VERTICES = 32768
EPSILON = 1e-06
SHRINK_BITS = 10
SHRINK = 2.0**-SHRINK_BITS
GROWTH_BITS = 17
CODES = 65000.0
ZERO_CODE = -32768
LOADS = 8
LOAD_SLOTS = KMAX // LOADS
TRIP = 16
SIDE = 512
OTHER, OWN = 0, 1
PARTS = ((0, 48), (48, 48), (96, 32))
PLANE = ((0, 1), (1, 0), (3, 0), (1, 1), (3, 1), (2, 0), (2, 1))
FLAT = sorted(
    ((i, j) for i in range(4) for j in range(4) if i or j), key=lambda s: min(s[0], 4 - s[0]) + min(s[1], 4 - s[1])
)
RELAYS = (
    *((0, i, z) for i, z in ((0, 1), (1, 0), (3, 0), (1, 1), (3, 1))),
    *((1, i, z) for i, z in ((0, 1), (1, 0), (3, 0))),
    *((0, i, z) for i, z in ((2, 0), (2, 1))),
    *((1, i, z) for i, z in ((1, 1), (3, 1), (2, 0), (2, 1))),
)
GROUPS = (
    ((0, 0), (0, 1), (0, 3), (1, 0), (3, 0)),
    ((1, 1), (1, 3), (3, 1), (3, 3)),
    ((2, 0), (0, 2), (2, 1), (1, 2)),
    ((2, 3), (3, 2), (2, 2)),
)


def place_of(step_x, step_y, step_z):
    return (step_x % 4 * 4 + step_y % 4) * 2 + step_z % 2


def row_of(x, z_lo, y):
    return x * 8 + z_lo * 4 + y


def densify(count_hbm, rows_hbm, cols_hbm, tiles_hbm, dense_ref, count_ref, rows_ref, cols_ref, tiles, small_sem, load_sem):
    core = lax.axis_index("col") % 2
    r = lax.axis_index("row")
    x, z_lo, y = r // 8, (r // 4) % 2, r % 4

    def load(part):
        slots = pl.ds(part * LOAD_SLOTS, LOAD_SLOTS)
        return pltpu.make_async_copy(tiles_hbm.at[0, 0, slots], tiles.at[slots], load_sem.at[part])

    small = (
        pltpu.make_async_copy(count_hbm, count_ref, small_sem.at[0]),
        pltpu.make_async_copy(rows_hbm, rows_ref, small_sem.at[1]),
        pltpu.make_async_copy(cols_hbm, cols_ref, small_sem.at[2]),
    )
    for copy in small:
        copy.start()
    for part in range(LOADS):
        load(part).start()

    @pl.loop(0, SRCS * TILE // 64)
    def _(block):
        rows = pl.ds(pl.multiple_of(block * 64, 64), 64)
        dense_ref[rows, :] = jnp.zeros((64, DESTS * TILE), jnp.bfloat16)

    for copy in small:
        copy.wait()
    count = count_ref[0, 0]
    for part in range(LOADS):
        load(part).wait()
        first = part * (LOAD_SLOTS // TRIP)

        @pl.loop(first, jnp.minimum((count + TRIP - 1) // TRIP, first + LOAD_SLOTS // TRIP))
        def _(trip):
            for inner in range(TRIP):
                slot = trip * TRIP + inner
                dest = rows_ref[0, 0, slot]
                row = cols_ref[0, 0, slot]
                steps = (((row >> 3) - x) & 3, (row - y) & 3, ((row >> 2) ^ z_lo) & 1)
                place = steps[0] * 8 + steps[1] * 2 + steps[2]
                side = 1 - ((dest ^ core) & 1)
                rows = pl.ds(pl.multiple_of(place * TILE, TILE), TILE)
                columns = pl.ds(pl.multiple_of(side * SIDE + (dest >> 1) * TILE, TILE), TILE)
                tile = tiles[slot].T
                dense_ref[rows, columns] += jnp.where(slot < count, tile, jnp.zeros_like(tile))


def levels_kernel(
    dense,
    depth_ref,
    ids_ref,
    paths,
    totals_ref,
    panel,
    depth,
    partial,
    from_core,
    codes,
    from_z,
    early,
    early_z,
    early_xy,
    last,
    last_z,
    last_xy,
    tile_send,
    tile_recv,
    core_send,
    core_recv,
    z_send,
    z_recv,
    norm_send,
    norm_recv,
):
    r = lax.axis_index("row")
    c = lax.axis_index("col")
    x, z_lo, y = r // 8, (r // 4) % 2, r % 4
    z_hi, core = c // 2, c % 2

    barrier = pltpu.get_barrier_semaphore()

    @pl.loop(1, N_ROW)
    def _(step):
        pl.semaphore_signal(
            barrier, inc=1, device_id={"row": (r + step) % N_ROW, "col": c}, device_id_type=MESH
        )

    @pl.loop(1, N_COL)
    def _(step):
        to = (c + step) % N_COL
        pl.semaphore_signal(barrier, inc=1, device_id={"row": r, "col": to}, device_id_type=MESH)
        pl.semaphore_signal(
            barrier, inc=1, device_id={"row": row_of(x, 1 - z_lo, y), "col": to}, device_id_type=MESH
        )

    def product(tiles, chunks, side):
        columns = slice(side * SIDE, (side + 1) * SIDE)
        total = None
        for step_x, step_y in chunks:
            index = step_x * 4 + step_y
            rows = slice(index * 2 * TILE, (index + 1) * 2 * TILE)
            source = jnp.concatenate([tiles[index * 2], tiles[index * 2 + 1]], axis=1)
            term = jnp.dot(source, dense[rows, columns], preferred_element_type=jnp.float32)
            total = term if total is None else total + term
        return total

    def part_of(buffer, place, part):
        start, size = PARTS[part]
        return panel.at[buffer, place, pl.ds(start, size)]

    def tile_copy(buffer, part, tile, to):
        there = place_of(*(i - j for i, j in zip(tile, to)))
        return pltpu.make_async_remote_copy(
            src_ref=part_of(buffer, place_of(*tile), part),
            dst_ref=part_of(buffer, there, part),
            send_sem=tile_send,
            recv_sem=tile_recv.at[buffer, part, there],
            device_id={"row": row_of((x + to[0]) % 4, (z_lo + to[2]) % 2, (y + to[1]) % 4), "col": c},
            device_id_type=MESH,
        )

    def wait_tile(buffer, part, tile):
        ref = part_of(buffer, place_of(*tile), part)
        pltpu.make_async_copy(ref, ref, tile_recv.at[buffer, part, place_of(*tile)]).wait()

    def at(part, along, across, z):
        return (along, across, z) if part == 0 else (across, along, z)

    def send_along(buffer, part, tile):
        for along in (1, 3, 2):
            tile_copy(buffer, part, tile, at(part, along, 0, 0)).start()

    def start_routed(buffer, part):
        for across, z in PLANE:
            tile_copy(buffer, part, (0, 0, 0), at(part, 0, across, z)).start()
        send_along(buffer, part, (0, 0, 0))

    def start_flat(buffer):
        tile_copy(buffer, 2, (0, 0, 0), (0, 0, 1)).start()
        for step in FLAT:
            tile_copy(buffer, 2, (0, 0, 0), (*step, 0)).start()

    def gather(buffer, wait_sends):
        with jax.named_scope("routed"):
            for part, across, z in RELAYS:
                wait_tile(buffer, part, at(part, 0, across, z))
                send_along(buffer, part, at(part, 0, across, z))
        with jax.named_scope("flat"):
            for step in FLAT:
                wait_tile(buffer, 2, (*step, 0))
                tile_copy(buffer, 2, (*step, 0), (0, 0, 1)).start()
        for number, group in enumerate(GROUPS):
            with jax.named_scope("wait_group_%d" % number):
                wait_group(buffer, group)
                if number == 0:
                    wait_sends()
            if number < len(GROUPS) - 1:
                with jax.named_scope("mm_group_%d" % number):
                    for side in range(2):
                        if number == 0:
                            partial[side] = product(panel.at[buffer], group, side)
                        else:
                            partial[side] += product(panel.at[buffer], group, side)

    def wait_group(buffer, steps):
        for step in steps:
            for z in range(2):
                if step[0]:
                    wait_tile(buffer, 0, (*step, z))
                if step[1]:
                    wait_tile(buffer, 1, (*step, z))
            wait_tile(buffer, 2, (*step, 1))

    def core_copy(buffer, half, part):
        columns = pl.ds(pl.multiple_of(part * TILE, TILE), TILE)
        return pltpu.make_async_remote_copy(
            src_ref=partial.at[OTHER, pl.ds(*PIECES[half]), columns],
            dst_ref=from_core.at[buffer, half, part, pl.ds(0, PIECES[half][1])],
            send_sem=core_send.at[half, part],
            recv_sem=core_recv.at[buffer, half, part],
            device_id={"row": r, "col": z_hi * 2 + 1 - core},
            device_id_type=MESH,
        )

    def z_copy(buffer, half, step):
        return pltpu.make_async_remote_copy(
            src_ref=codes.at[half, step - 1, pl.ds(0, PIECES[half][1])],
            dst_ref=from_z.at[buffer, half, step - 1, pl.ds(0, PIECES[half][1])],
            send_sem=z_send.at[half, step - 1],
            recv_sem=z_recv.at[buffer, half, step - 1],
            device_id={"row": r, "col": ((z_hi + step) % 4) * 2 + core},
            device_id_type=MESH,
        )

    def code_scale(level):
        before = (jnp.zeros((1, PANEL), jnp.int32) + (level - 1)).astype(jnp.float32)
        steps = CODES / (GROWTH_BITS * (before + 1.0) + 0.5)
        middle = 0.5 * (GROWTH_BITS + (GROWTH_BITS - 2 * SHRINK_BITS) * before)
        return steps, middle

    def both_cores(buffer, half, part):
        core_copy(buffer, half, part).wait_recv()
        columns = pl.ds(pl.multiple_of(part * TILE, TILE), TILE)
        return partial[OWN, pl.ds(*PIECES[half]), columns] + from_core[buffer, half, part, : PIECES[half][1]]

    def combine(level, buffer, half):
        steps, middle = code_scale(level)
        for step in (2, 1, 3):
            value = both_cores(buffer, half, (z_hi + step) % 4)
            code = jnp.round((jnp.log2(jnp.maximum(value, 2.0**-60)) - middle) * steps).astype(jnp.int32)
            codes[half, step - 1, : PIECES[half][1]] = jnp.where(value > 0.0, code, ZERO_CODE).astype(jnp.int16)
            z_copy(buffer, half, step).start()

    def finish(level, buffer, half):
        steps, middle = code_scale(level)
        mine = both_cores(buffer, half, z_hi)
        for step in (1, 3, 2):
            z_copy(buffer, half, step).wait_recv()
            code = from_z[buffer, half, step - 1, : PIECES[half][1]].astype(jnp.int32)
            value = jnp.exp2(code.astype(jnp.float32) * (1.0 / steps) + middle)
            mine = mine + jnp.where(code == ZERO_CODE, 0.0, value)
        rows = pl.ds(*PIECES[half])
        raw = jnp.where(depth[rows] >= level, mine, 0.0)
        paths[level - 1, rows] = raw
        return raw

    def wait_sends():
        for half in range(2):
            for part in range(4):
                core_copy(0, half, part).wait_send()
            for step in (1, 2, 3):
                z_copy(0, half, step).wait_send()

    def wait_tile_sends(buffer):
        sent = panel.at[buffer, pl.ds(0, SRCS - 1)]
        pltpu.make_async_copy(sent, sent, tile_send).wait()

    def reduce_level(level, buffer, out, side_product, drain, keep, early_core):
        def other_side():
            partial[OTHER] = side_product(OTHER)
            for half in range(2):
                for step in (2, 1, 3, 0):
                    core_copy(buffer, half, (z_hi + step) % 4).start()

        def own_side():
            partial[OWN] = side_product(OWN)

        def combine_both():
            for half in range(2):
                combine(level, buffer, half)

        def own_first():
            own_side()
            combine_both()
            other_side()

        def other_first():
            other_side()
            own_side()
            combine_both()

        with jax.named_scope("mm_last"):
            if early_core is None:
                other_first()
            else:
                pl.when(core == early_core)(other_first)
                pl.when(core != early_core)(own_first)
            drain()
        for half in range(2):
            with jax.named_scope("finish_%d" % half):
                raw = finish(level, buffer, half)
                if out is not None:
                    panel[out, 0, pl.ds(*PIECES[half])] = (raw * SHRINK).astype(jnp.bfloat16)
                    start_routed(out, half)
                    if half == 1:
                        start_flat(out)
        with jax.named_scope("squares"):
            by_vertex = paths[level - 1].T
            keep(jnp.sum(by_vertex * by_vertex, axis=0, keepdims=True))
            paths[level - 1] = by_vertex

    mine_z = z_lo * N_COL + c
    mine_xy = x * 4 + y

    def z_peer(step):
        index = (mine_z + step) % 16
        return index, {"row": row_of(x, index // 8, y), "col": index % 8}

    def xy_peer(step):
        index = (mine_xy + step) % 16
        return index, {"row": row_of(index // 4, z_lo, index % 4), "col": c}

    def norm_start(which, source, slots, peer, mine):
        slots[mine] = source[...]

        @pl.loop(1, 16)
        def _(step):
            pltpu.make_async_remote_copy(
                src_ref=source,
                dst_ref=slots.at[mine],
                send_sem=norm_send.at[which],
                recv_sem=norm_recv.at[which, mine],
                device_id=peer(step)[1],
                device_id_type=MESH,
            ).start()

    def norm_wait(which, slots, peer):
        @pl.loop(1, 16)
        def _(step):
            slot = slots.at[peer(step)[0]]
            pltpu.make_async_copy(slot, slot, norm_recv.at[which, peer(step)[0]]).wait()

        sent = slots.at[pl.ds(0, 15)]
        pltpu.make_async_copy(sent, sent, norm_send.at[which]).wait()
        return jnp.sum(slots[...], axis=0)

    with jax.named_scope("onehot"):
        early[...] = jnp.zeros_like(early)
        depth[...] = jnp.broadcast_to(depth_ref[...], (TILE, PANEL)).astype(jnp.float32).T.astype(jnp.int32)
        ids = jnp.broadcast_to(ids_ref[...], (TILE, PANEL)).astype(jnp.float32).T.astype(jnp.int32)
        offsets = ids - lax.broadcasted_iota(jnp.int32, (PANEL, TILE), 1)

        @pl.loop(0, SRCS // 4)
        def _(quad):
            for inner in range(4):
                step_x, step_y = quad // 2, quad % 2 * 2 + inner // 2
                row = row_of((x + step_x) % 4, (z_lo + inner) % 2, (y + step_y) % 4)
                hit = offsets == (row * N_COL + c) * TILE
                panel[0, quad * 4 + inner] = hit.astype(jnp.float32).astype(jnp.bfloat16)

    def first_product(side):
        total = product(panel.at[0], [(i, j) for i in range(4) for j in range(4)], side)
        if side == OTHER:
            with jax.named_scope("barrier"):
                pl.semaphore_wait(barrier, N_ROW - 1 + 2 * (N_COL - 1))
        return total

    def keep_early(level):
        def keep(squares):
            early[pl.ds(level - 1, 1), :] = squares

        return keep

    reduce_level(1, 1, 1, first_product, lambda: None, keep_early(1), None)

    @pl.loop(2, LEVELS)
    def _(level):
        buffer = (level + 1) % 2
        gather(buffer, wait_sends)
        reduce_level(
            level,
            1 - buffer,
            1 - buffer,
            lambda side: partial[side] + product(panel.at[buffer], GROUPS[-1], side),
            lambda: wait_tile_sends(buffer),
            keep_early(level),
            1,
        )

    norm_start(0, early, early_z, z_peer, mine_z)
    buffer = (LEVELS + 1) % 2

    def middle_of_last():
        wait_sends()
        early[...] = norm_wait(0, early_z, z_peer)
        norm_start(1, early, early_xy, xy_peer, mine_xy)

    gather(buffer, middle_of_last)

    def keep_last(squares):
        last[...] = squares

    reduce_level(
        LEVELS,
        1 - buffer,
        None,
        lambda side: partial[side] + product(panel.at[buffer], GROUPS[-1], side),
        lambda: wait_tile_sends(buffer),
        keep_last,
        1,
    )

    with jax.named_scope("norm_z"):
        norm_start(2, last, last_z, z_peer, mine_z)
        wait_sends()
        totals = norm_wait(1, early_xy, xy_peer)
        last[...] = norm_wait(2, last_z, z_peer)
    with jax.named_scope("norm_xy"):
        norm_start(3, last, last_xy, xy_peer, mine_xy)
        last_total = norm_wait(3, last_xy, xy_peer)

    totals_ref[0 : LEVELS - 1, :] = totals[0 : LEVELS - 1]
    totals_ref[LEVELS - 1 : LEVELS, :] = last_total


def outputs(ids_ref, paths, totals, sums_ref, logs_ref):
    position = lax.axis_index("row") * N_COL + lax.axis_index("col")
    vertex = position * TILE + lax.broadcasted_iota(jnp.int32, (TILE, PANEL), 0)
    sums = (vertex == ids_ref[...]).astype(jnp.float32)
    kappa = jnp.ones((1, PANEL), jnp.float32)
    for level in range(LEVELS):
        mean_square = totals[level : level + 1] / VERTICES / kappa / kappa + EPSILON
        scale = kappa * jnp.sqrt(mean_square)
        sums = sums + paths[level] * (1.0 / scale)
        logs_ref[level : level + 1, :] = 0.5 * jnp.log(mean_square)
        kappa = scale * SHRINK
    sums_ref[...] = sums


def local(adj_tiles, tile_rows, tile_cols, tile_count, tile_depth, source_ids):
    hbm = pl.BlockSpec(memory_space=pltpu.HBM)
    vmem = pl.BlockSpec(memory_space=pltpu.VMEM)
    dense = pl.pallas_call(
        densify,
        out_shape=pltpu.VMEM((SRCS * TILE, DESTS * TILE), jnp.bfloat16),
        in_specs=[hbm, hbm, hbm, hbm],
        out_specs=vmem,
        scratch_shapes=[
            pltpu.SMEM((1, 1), jnp.int32),
            pltpu.SMEM((1, 1, KMAX), jnp.int32),
            pltpu.SMEM((1, 1, KMAX), jnp.int32),
            pltpu.VMEM((KMAX, TILE, TILE), jnp.bfloat16),
            pltpu.SemaphoreType.DMA((3,)),
            pltpu.SemaphoreType.DMA((LOADS,)),
        ],
        compiler_params=pltpu.CompilerParams(vmem_limit_bytes=53 * 2**20),
        name="densify",
    )(tile_count, tile_rows, tile_cols, adj_tiles)
    ids = source_ids.reshape(1, PANEL)
    paths, totals = pl.pallas_call(
        levels_kernel,
        out_shape=(
            pltpu.VMEM((LEVELS, TILE, PANEL), jnp.float32),
            pltpu.VMEM((LEVELS, PANEL), jnp.float32),
        ),
        in_specs=[vmem, vmem, vmem],
        out_specs=(vmem, vmem),
        scratch_shapes=[
            pltpu.VMEM((2, SRCS, TILE, PANEL), jnp.bfloat16),
            pltpu.VMEM((PANEL, TILE), jnp.int32),
            pltpu.VMEM((2, PANEL, SIDE), jnp.float32),
            pltpu.VMEM((2, 2, 4, LONGEST, TILE), jnp.float32),
            pltpu.VMEM((2, 3, LONGEST, PANEL), jnp.int16),
            pltpu.VMEM((2, 2, 3, LONGEST, PANEL), jnp.int16),
            pltpu.VMEM((8, PANEL), jnp.float32),
            pltpu.VMEM((16, 8, PANEL), jnp.float32),
            pltpu.VMEM((16, 8, PANEL), jnp.float32),
            pltpu.VMEM((1, PANEL), jnp.float32),
            pltpu.VMEM((16, 1, PANEL), jnp.float32),
            pltpu.VMEM((16, 1, PANEL), jnp.float32),
            pltpu.SemaphoreType.DMA,
            pltpu.SemaphoreType.DMA((2, 3, SRCS)),
            pltpu.SemaphoreType.DMA((2, 4)),
            pltpu.SemaphoreType.DMA((2, 2, 4)),
            pltpu.SemaphoreType.DMA((2, 3)),
            pltpu.SemaphoreType.DMA((2, 2, 3)),
            pltpu.SemaphoreType.DMA((4,)),
            pltpu.SemaphoreType.DMA((4, 16)),
        ],
        compiler_params=pltpu.CompilerParams(
            collective_id=0, has_side_effects=True, vmem_limit_bytes=32 * 2**20
        ),
        name="levels",
    )(dense, tile_depth, ids)
    return pl.pallas_call(
        outputs,
        out_shape=(
            pltpu.HBM((TILE, PANEL), jnp.float32),
            pltpu.HBM((LEVELS, PANEL), jnp.float32),
        ),
        in_specs=[vmem, vmem, vmem],
        out_specs=(vmem, vmem),
        compiler_params=pltpu.CompilerParams(vmem_limit_bytes=32 * 2**20),
        name="outputs",
    )(ids, paths, totals)


def solution(mesh):
    in_specs = (
        P("row", "col", None, None, None),
        P("row", "col", None),
        P("row", "col", None),
        P("row", "col"),
        P(("row", "col"), None),
        P(),
    )
    out_specs = (P(("row", "col"), None), P())
    return jax.shard_map(local, mesh=mesh, in_specs=in_specs, out_specs=out_specs, check_vma=False)
```

```python
import jax
import jax.numpy as jnp
from jax import lax
from jax.experimental import pallas as pl
from jax.experimental.pallas import tpu as pltpu
from jax.sharding import PartitionSpec as P

MESH = pl.DeviceIdType.MESH
TILE = 128
PIECES = ((0, 48), (48, 80))
LONGEST = 80
PANEL = 128
LEVELS = 6
KMAX = 128
DESTS = 8
SRCS = 32
N_ROW = 32
N_COL = 8
VERTICES = 32768
EPSILON = 1e-06
SHRINK_BITS = 10
SHRINK = 2.0**-SHRINK_BITS
GROWTH_BITS = 17
CODES = 65000.0
ZERO_CODE = -32768
LOADS = 8
LOAD_SLOTS = KMAX // LOADS
TRIP = 16
SIDE = 512
OTHER, OWN = 0, 1
PARTS = ((0, 48), (48, 48), (96, 32))
PLANE = ((0, 1), (1, 0), (3, 0), (1, 1), (3, 1), (2, 0), (2, 1))
FLAT = sorted(
    ((i, j) for i in range(4) for j in range(4) if i or j), key=lambda s: min(s[0], 4 - s[0]) + min(s[1], 4 - s[1])
)
RELAYS = (
    *((0, i, z) for i, z in ((0, 1), (1, 0), (3, 0), (1, 1), (3, 1))),
    *((1, i, z) for i, z in ((0, 1), (1, 0), (3, 0))),
    *((0, i, z) for i, z in ((2, 0), (2, 1))),
    *((1, i, z) for i, z in ((1, 1), (3, 1), (2, 0), (2, 1))),
)
GROUPS = (
    ((0, 0), (0, 1), (0, 3), (1, 0), (3, 0)),
    ((1, 1), (1, 3), (3, 1), (3, 3)),
    ((2, 0), (0, 2), (2, 1), (1, 2)),
    ((2, 3), (3, 2), (2, 2)),
)


def place_of(step_x, step_y, step_z):
    return (step_x % 4 * 4 + step_y % 4) * 2 + step_z % 2


def row_of(x, z_lo, y):
    return x * 8 + z_lo * 4 + y


def densify(count_hbm, rows_hbm, cols_hbm, tiles_hbm, dense_ref, count_ref, rows_ref, cols_ref, tiles, small_sem, load_sem):
    core = lax.axis_index("col") % 2
    r = lax.axis_index("row")
    x, z_lo, y = r // 8, (r // 4) % 2, r % 4

    def load(part):
        slots = pl.ds(part * LOAD_SLOTS, LOAD_SLOTS)
        return pltpu.make_async_copy(tiles_hbm.at[0, 0, slots], tiles.at[slots], load_sem.at[part])

    small = (
        pltpu.make_async_copy(count_hbm, count_ref, small_sem.at[0]),
        pltpu.make_async_copy(rows_hbm, rows_ref, small_sem.at[1]),
        pltpu.make_async_copy(cols_hbm, cols_ref, small_sem.at[2]),
    )
    for copy in small:
        copy.start()
    for part in range(LOADS):
        load(part).start()

    @pl.loop(0, SRCS * TILE // 64)
    def _(block):
        rows = pl.ds(pl.multiple_of(block * 64, 64), 64)
        dense_ref[rows, :] = jnp.zeros((64, DESTS * TILE), jnp.bfloat16)

    for copy in small:
        copy.wait()
    count = count_ref[0, 0]
    for part in range(LOADS):
        load(part).wait()
        first = part * (LOAD_SLOTS // TRIP)

        @pl.loop(first, jnp.minimum((count + TRIP - 1) // TRIP, first + LOAD_SLOTS // TRIP))
        def _(trip):
            for inner in range(TRIP):
                slot = trip * TRIP + inner
                dest = rows_ref[0, 0, slot]
                row = cols_ref[0, 0, slot]
                steps = (((row >> 3) - x) & 3, (row - y) & 3, ((row >> 2) ^ z_lo) & 1)
                place = steps[0] * 8 + steps[1] * 2 + steps[2]
                side = 1 - ((dest ^ core) & 1)
                rows = pl.ds(pl.multiple_of(place * TILE, TILE), TILE)
                columns = pl.ds(pl.multiple_of(side * SIDE + (dest >> 1) * TILE, TILE), TILE)
                tile = tiles[slot].T
                dense_ref[rows, columns] += jnp.where(slot < count, tile, jnp.zeros_like(tile))


def levels_kernel(
    dense,
    depth_ref,
    ids_ref,
    paths,
    totals_ref,
    panel,
    depth,
    partial,
    from_core,
    codes,
    from_z,
    early,
    early_z,
    early_xy,
    last,
    last_z,
    last_xy,
    tile_send,
    tile_recv,
    core_send,
    core_recv,
    z_send,
    z_recv,
    norm_send,
    norm_recv,
):
    r = lax.axis_index("row")
    c = lax.axis_index("col")
    x, z_lo, y = r // 8, (r // 4) % 2, r % 4
    z_hi, core = c // 2, c % 2

    barrier = pltpu.get_barrier_semaphore()

    greeted = [(i, j, k, 0) for i in range(4) for j in range(4) for k in range(2) if i or j or k]
    greeted += [(0, 0, k, m) for k in range(2) for m in range(1, N_COL)]

    def hops(steps):
        return sum(min(i, 4 - i) for i in steps[:2]) + steps[2] + 2 * min(steps[3] // 2, 4 - steps[3] // 2)

    for i, j, k, m in sorted(greeted, key=hops, reverse=True):
        to = {"row": row_of((x + i) % 4, (z_lo + k) % 2, (y + j) % 4), "col": (c + m) % N_COL}
        pl.semaphore_signal(barrier, inc=1, device_id=to, device_id_type=MESH)

    def product(tiles, chunks, side):
        columns = slice(side * SIDE, (side + 1) * SIDE)
        total = None
        for step_x, step_y in chunks:
            index = step_x * 4 + step_y
            rows = slice(index * 2 * TILE, (index + 1) * 2 * TILE)
            source = jnp.concatenate([tiles[index * 2], tiles[index * 2 + 1]], axis=1)
            term = jnp.dot(source, dense[rows, columns], preferred_element_type=jnp.float32)
            total = term if total is None else total + term
        return total

    def part_of(buffer, place, part):
        start, size = PARTS[part]
        return panel.at[buffer, place, pl.ds(start, size)]

    def tile_copy(buffer, part, tile, to):
        there = place_of(*(i - j for i, j in zip(tile, to)))
        return pltpu.make_async_remote_copy(
            src_ref=part_of(buffer, place_of(*tile), part),
            dst_ref=part_of(buffer, there, part),
            send_sem=tile_send,
            recv_sem=tile_recv.at[buffer, part, there],
            device_id={"row": row_of((x + to[0]) % 4, (z_lo + to[2]) % 2, (y + to[1]) % 4), "col": c},
            device_id_type=MESH,
        )

    def wait_tile(buffer, part, tile):
        ref = part_of(buffer, place_of(*tile), part)
        pltpu.make_async_copy(ref, ref, tile_recv.at[buffer, part, place_of(*tile)]).wait()

    def at(part, along, across, z):
        return (along, across, z) if part == 0 else (across, along, z)

    def send_along(buffer, part, tile):
        for along in (1, 3, 2):
            tile_copy(buffer, part, tile, at(part, along, 0, 0)).start()

    def start_routed(buffer, part):
        for across, z in PLANE:
            tile_copy(buffer, part, (0, 0, 0), at(part, 0, across, z)).start()
        send_along(buffer, part, (0, 0, 0))

    def start_flat(buffer):
        tile_copy(buffer, 2, (0, 0, 0), (0, 0, 1)).start()
        for step in FLAT:
            tile_copy(buffer, 2, (0, 0, 0), (*step, 0)).start()

    def gather(buffer, wait_sends):
        with jax.named_scope("routed"):
            for part, across, z in RELAYS:
                wait_tile(buffer, part, at(part, 0, across, z))
                send_along(buffer, part, at(part, 0, across, z))
        with jax.named_scope("flat"):
            for step in FLAT:
                wait_tile(buffer, 2, (*step, 0))
                tile_copy(buffer, 2, (*step, 0), (0, 0, 1)).start()
        for number, group in enumerate(GROUPS):
            with jax.named_scope("wait_group_%d" % number):
                wait_group(buffer, group)
                if number == 0:
                    wait_sends()
            if number < len(GROUPS) - 1:
                with jax.named_scope("mm_group_%d" % number):
                    for side in range(2):
                        if number == 0:
                            partial[side] = product(panel.at[buffer], group, side)
                        else:
                            partial[side] += product(panel.at[buffer], group, side)

    def wait_group(buffer, steps):
        for step in steps:
            for z in range(2):
                if step[0]:
                    wait_tile(buffer, 0, (*step, z))
                if step[1]:
                    wait_tile(buffer, 1, (*step, z))
            wait_tile(buffer, 2, (*step, 1))

    def core_copy(buffer, half, part):
        columns = pl.ds(pl.multiple_of(part * TILE, TILE), TILE)
        return pltpu.make_async_remote_copy(
            src_ref=partial.at[OTHER, pl.ds(*PIECES[half]), columns],
            dst_ref=from_core.at[buffer, half, part, pl.ds(0, PIECES[half][1])],
            send_sem=core_send.at[half, part],
            recv_sem=core_recv.at[buffer, half, part],
            device_id={"row": r, "col": z_hi * 2 + 1 - core},
            device_id_type=MESH,
        )

    def z_copy(buffer, half, step):
        return pltpu.make_async_remote_copy(
            src_ref=codes.at[half, step - 1, pl.ds(0, PIECES[half][1])],
            dst_ref=from_z.at[buffer, half, step - 1, pl.ds(0, PIECES[half][1])],
            send_sem=z_send.at[half, step - 1],
            recv_sem=z_recv.at[buffer, half, step - 1],
            device_id={"row": r, "col": ((z_hi + step) % 4) * 2 + core},
            device_id_type=MESH,
        )

    def code_scale(level):
        before = (jnp.zeros((1, PANEL), jnp.int32) + (level - 1)).astype(jnp.float32)
        steps = CODES / (GROWTH_BITS * (before + 1.0) + 0.5)
        middle = 0.5 * (GROWTH_BITS + (GROWTH_BITS - 2 * SHRINK_BITS) * before)
        return steps, middle

    def both_cores(buffer, half, part):
        core_copy(buffer, half, part).wait_recv()
        columns = pl.ds(pl.multiple_of(part * TILE, TILE), TILE)
        return partial[OWN, pl.ds(*PIECES[half]), columns] + from_core[buffer, half, part, : PIECES[half][1]]

    def combine(level, buffer, half):
        steps, middle = code_scale(level)
        for step in (2, 1, 3):
            value = both_cores(buffer, half, (z_hi + step) % 4)
            code = jnp.round((jnp.log2(jnp.maximum(value, 2.0**-60)) - middle) * steps).astype(jnp.int32)
            codes[half, step - 1, : PIECES[half][1]] = jnp.where(value > 0.0, code, ZERO_CODE).astype(jnp.int16)
            z_copy(buffer, half, step).start()

    def finish(level, buffer, half):
        steps, middle = code_scale(level)
        mine = both_cores(buffer, half, z_hi)
        for step in (1, 3, 2):
            z_copy(buffer, half, step).wait_recv()
            code = from_z[buffer, half, step - 1, : PIECES[half][1]].astype(jnp.int32)
            value = jnp.exp2(code.astype(jnp.float32) * (1.0 / steps) + middle)
            mine = mine + jnp.where(code == ZERO_CODE, 0.0, value)
        rows = pl.ds(*PIECES[half])
        raw = jnp.where(depth[rows] >= level, mine, 0.0)
        paths[level - 1, rows] = raw
        return raw

    def wait_sends():
        for half in range(2):
            for part in range(4):
                core_copy(0, half, part).wait_send()
            for step in (1, 2, 3):
                z_copy(0, half, step).wait_send()

    def wait_tile_sends(buffer):
        sent = panel.at[buffer, pl.ds(0, SRCS - 1)]
        pltpu.make_async_copy(sent, sent, tile_send).wait()

    def reduce_level(level, buffer, out, side_product, drain, keep, early_core):
        def other_side():
            partial[OTHER] = side_product(OTHER)
            for half in range(2):
                for step in (2, 1, 3, 0):
                    core_copy(buffer, half, (z_hi + step) % 4).start()

        def own_side():
            partial[OWN] = side_product(OWN)

        def combine_both():
            for half in range(2):
                combine(level, buffer, half)

        def own_first():
            own_side()
            combine_both()
            other_side()

        def other_first():
            other_side()
            own_side()
            combine_both()

        with jax.named_scope("mm_last"):
            if early_core is None:
                other_first()
            else:
                pl.when(core == early_core)(other_first)
                pl.when(core != early_core)(own_first)
            drain()
        for half in range(2):
            with jax.named_scope("finish_%d" % half):
                raw = finish(level, buffer, half)
                if out is not None:
                    panel[out, 0, pl.ds(*PIECES[half])] = (raw * SHRINK).astype(jnp.bfloat16)
                    start_routed(out, half)
                    if half == 1:
                        start_flat(out)
        with jax.named_scope("squares"):
            by_vertex = paths[level - 1].T
            keep(jnp.sum(by_vertex * by_vertex, axis=0, keepdims=True))
            paths[level - 1] = by_vertex

    mine_z = z_lo * N_COL + c
    mine_xy = x * 4 + y

    def z_peer(step):
        index = (mine_z + step) % 16
        return index, {"row": row_of(x, index // 8, y), "col": index % 8}

    def xy_peer(step):
        index = (mine_xy + step) % 16
        return index, {"row": row_of(index // 4, z_lo, index % 4), "col": c}

    def norm_start(which, source, slots, peer, mine):
        slots[mine] = source[...]

        @pl.loop(1, 16)
        def _(step):
            pltpu.make_async_remote_copy(
                src_ref=source,
                dst_ref=slots.at[mine],
                send_sem=norm_send.at[which],
                recv_sem=norm_recv.at[which, mine],
                device_id=peer(step)[1],
                device_id_type=MESH,
            ).start()

    def norm_wait(which, slots, peer):
        @pl.loop(1, 16)
        def _(step):
            slot = slots.at[peer(step)[0]]
            pltpu.make_async_copy(slot, slot, norm_recv.at[which, peer(step)[0]]).wait()

        sent = slots.at[pl.ds(0, 15)]
        pltpu.make_async_copy(sent, sent, norm_send.at[which]).wait()
        return jnp.sum(slots[...], axis=0)

    with jax.named_scope("onehot"):
        early[...] = jnp.zeros_like(early)
        depth[...] = jnp.broadcast_to(depth_ref[...], (TILE, PANEL)).astype(jnp.float32).T.astype(jnp.int32)
        ids = jnp.broadcast_to(ids_ref[...], (TILE, PANEL)).astype(jnp.float32).T.astype(jnp.int32)
        offsets = ids - lax.broadcasted_iota(jnp.int32, (PANEL, TILE), 1)

        @pl.loop(0, SRCS // 4)
        def _(quad):
            for inner in range(4):
                step_x, step_y = quad // 2, quad % 2 * 2 + inner // 2
                row = row_of((x + step_x) % 4, (z_lo + inner) % 2, (y + step_y) % 4)
                hit = offsets == (row * N_COL + c) * TILE
                panel[0, quad * 4 + inner] = hit.astype(jnp.float32).astype(jnp.bfloat16)

    def first_product(side):
        total = product(panel.at[0], [(i, j) for i in range(4) for j in range(4)], side)
        if side == OTHER:
            with jax.named_scope("barrier"):
                pl.semaphore_wait(barrier, N_ROW - 1 + 2 * (N_COL - 1))
        return total

    def keep_early(level):
        def keep(squares):
            early[pl.ds(level - 1, 1), :] = squares

        return keep

    reduce_level(1, 1, 1, first_product, lambda: None, keep_early(1), None)

    @pl.loop(2, LEVELS)
    def _(level):
        buffer = (level + 1) % 2
        gather(buffer, wait_sends)
        reduce_level(
            level,
            1 - buffer,
            1 - buffer,
            lambda side: partial[side] + product(panel.at[buffer], GROUPS[-1], side),
            lambda: wait_tile_sends(buffer),
            keep_early(level),
            1,
        )

    norm_start(0, early, early_z, z_peer, mine_z)
    buffer = (LEVELS + 1) % 2

    def middle_of_last():
        wait_sends()
        early[...] = norm_wait(0, early_z, z_peer)
        norm_start(1, early, early_xy, xy_peer, mine_xy)

    gather(buffer, middle_of_last)

    def keep_last(squares):
        last[...] = squares

    reduce_level(
        LEVELS,
        1 - buffer,
        None,
        lambda side: partial[side] + product(panel.at[buffer], GROUPS[-1], side),
        lambda: wait_tile_sends(buffer),
        keep_last,
        1,
    )

    with jax.named_scope("norm_z"):
        norm_start(2, last, last_z, z_peer, mine_z)
        wait_sends()
        totals = norm_wait(1, early_xy, xy_peer)
        last[...] = norm_wait(2, last_z, z_peer)
    with jax.named_scope("norm_xy"):
        norm_start(3, last, last_xy, xy_peer, mine_xy)
        last_total = norm_wait(3, last_xy, xy_peer)

    totals_ref[0 : LEVELS - 1, :] = totals[0 : LEVELS - 1]
    totals_ref[LEVELS - 1 : LEVELS, :] = last_total


def outputs(ids_ref, paths, totals, sums_ref, logs_ref):
    position = lax.axis_index("row") * N_COL + lax.axis_index("col")
    vertex = position * TILE + lax.broadcasted_iota(jnp.int32, (TILE, PANEL), 0)
    sums = (vertex == ids_ref[...]).astype(jnp.float32)
    kappa = jnp.ones((1, PANEL), jnp.float32)
    for level in range(LEVELS):
        mean_square = totals[level : level + 1] / VERTICES / kappa / kappa + EPSILON
        scale = kappa * jnp.sqrt(mean_square)
        sums = sums + paths[level] * (1.0 / scale)
        logs_ref[level : level + 1, :] = 0.5 * jnp.log(mean_square)
        kappa = scale * SHRINK
    sums_ref[...] = sums


def local(adj_tiles, tile_rows, tile_cols, tile_count, tile_depth, source_ids):
    hbm = pl.BlockSpec(memory_space=pltpu.HBM)
    vmem = pl.BlockSpec(memory_space=pltpu.VMEM)
    dense = pl.pallas_call(
        densify,
        out_shape=pltpu.VMEM((SRCS * TILE, DESTS * TILE), jnp.bfloat16),
        in_specs=[hbm, hbm, hbm, hbm],
        out_specs=vmem,
        scratch_shapes=[
            pltpu.SMEM((1, 1), jnp.int32),
            pltpu.SMEM((1, 1, KMAX), jnp.int32),
            pltpu.SMEM((1, 1, KMAX), jnp.int32),
            pltpu.VMEM((KMAX, TILE, TILE), jnp.bfloat16),
            pltpu.SemaphoreType.DMA((3,)),
            pltpu.SemaphoreType.DMA((LOADS,)),
        ],
        compiler_params=pltpu.CompilerParams(vmem_limit_bytes=53 * 2**20),
        name="densify",
    )(tile_count, tile_rows, tile_cols, adj_tiles)
    ids = source_ids.reshape(1, PANEL)
    paths, totals = pl.pallas_call(
        levels_kernel,
        out_shape=(
            pltpu.VMEM((LEVELS, TILE, PANEL), jnp.float32),
            pltpu.VMEM((LEVELS, PANEL), jnp.float32),
        ),
        in_specs=[vmem, vmem, vmem],
        out_specs=(vmem, vmem),
        scratch_shapes=[
            pltpu.VMEM((2, SRCS, TILE, PANEL), jnp.bfloat16),
            pltpu.VMEM((PANEL, TILE), jnp.int32),
            pltpu.VMEM((2, PANEL, SIDE), jnp.float32),
            pltpu.VMEM((2, 2, 4, LONGEST, TILE), jnp.float32),
            pltpu.VMEM((2, 3, LONGEST, PANEL), jnp.int16),
            pltpu.VMEM((2, 2, 3, LONGEST, PANEL), jnp.int16),
            pltpu.VMEM((8, PANEL), jnp.float32),
            pltpu.VMEM((16, 8, PANEL), jnp.float32),
            pltpu.VMEM((16, 8, PANEL), jnp.float32),
            pltpu.VMEM((1, PANEL), jnp.float32),
            pltpu.VMEM((16, 1, PANEL), jnp.float32),
            pltpu.VMEM((16, 1, PANEL), jnp.float32),
            pltpu.SemaphoreType.DMA,
            pltpu.SemaphoreType.DMA((2, 3, SRCS)),
            pltpu.SemaphoreType.DMA((2, 4)),
            pltpu.SemaphoreType.DMA((2, 2, 4)),
            pltpu.SemaphoreType.DMA((2, 3)),
            pltpu.SemaphoreType.DMA((2, 2, 3)),
            pltpu.SemaphoreType.DMA((4,)),
            pltpu.SemaphoreType.DMA((4, 16)),
        ],
        compiler_params=pltpu.CompilerParams(
            collective_id=0, has_side_effects=True, vmem_limit_bytes=32 * 2**20
        ),
        name="levels",
    )(dense, tile_depth, ids)
    return pl.pallas_call(
        outputs,
        out_shape=(
            pltpu.HBM((TILE, PANEL), jnp.float32),
            pltpu.HBM((LEVELS, PANEL), jnp.float32),
        ),
        in_specs=[vmem, vmem, vmem],
        out_specs=(vmem, vmem),
        compiler_params=pltpu.CompilerParams(vmem_limit_bytes=32 * 2**20),
        name="outputs",
    )(ids, paths, totals)


def solution(mesh):
    in_specs = (
        P("row", "col", None, None, None),
        P("row", "col", None),
        P("row", "col", None),
        P("row", "col"),
        P(("row", "col"), None),
        P(),
    )
    out_specs = (P(("row", "col"), None), P())
    return jax.shard_map(local, mesh=mesh, in_specs=in_specs, out_specs=out_specs, check_vma=False)
```
